32 devices in a mesh: gx: 4 (over y, core), gy: 4 (over z), gz: 2 (over x).
Axes of the slice: x: 2, y: 2, z: 4, core: 2. Of those that a mesh axis runs over, the one named last changes fastest.
Arguments:
- positions: float32 [3, 4, 8, 16, 128], P(None, 'gx', 'gy', 'gz'), may hold values from 0 to 1
- velocities: float32 [3, 4, 8, 16, 128], P(None, 'gx', 'gy', 'gz'), may hold values from -6 to 6
- occupancy: int32 [4, 8, 16], P('gx', 'gy', 'gz'), may hold values from 0 to 128, as said below
- mover_pos: float32 [3, 12, 4, 2, 128], P(None, 'gx', 'gy', 'gz'), may hold values from 0 to 1
- mover_vel: float32 [3, 12, 4, 2, 128], P(None, 'gx', 'gy', 'gz'), may hold values from -6 to 6
- mover_count: int32 [12, 4, 2], P('gx', 'gy', 'gz'), may hold values from 1 to 128
- mover_owner: int32 [12, 4, 2], P('gx', 'gy', 'gz'), may hold values from 0 to 3, as said below
- mover_cell: int32 [12, 4, 2], P('gx', 'gy', 'gz'), may hold values from 0 to 15, as said below
Outputs:
- new_positions: float32 [3, 4, 8, 16, 128], P(None, 'gx', 'gy', 'gz')
- new_velocities: float32 [3, 4, 8, 16, 128], P(None, 'gx', 'gy', 'gz')
The draws below stay inside these ranges and needn't reach their ends.
Inputs may be any that keep to these rules, and one draw needn't show every extreme that they name: `mover_owner`: all leaving blocks of one device go to one owner in the device's own line along gx; at most 6 blocks arrive at one device, and in every draw some device takes 2 * 3 and some takes none. `mover_cell`: the cells named by the blocks that arrive at one device are distinct, and their occupancy is 0. Exactly 6 cells of each device have occupancy 0; every other cell holds 32 or more particles, and one cell of each device holds 128.
All inputs are finite; a program needn't handle non-finite values.
Results may differ from the reference program's by a relative error of at most 0.0001.
Values sent between devices are 32-bit elements; how exact they have to be, the bound alone decides.
A program may use at most 64 MiB of HBM per device.

```python
import math
import jax
import jax.numpy as jnp
from jax import lax

CX = 1
CY = 2
CZ = 8
SLOTS = 128
CAP = 3
NX = 4
NY = 8
NZ = 16
MOVERS = 12
N_GX = 4
N_GY = 4
N_GZ = 2


def column_plan(key):
    cell_total = CX * CY * CZ

    def one_column(column_key):
        keys = jax.random.split(column_key, 5)
        sigma = jax.random.permutation(keys[0], N_GX)
        heavy = jax.random.randint(keys[1], (N_GX // 2,), 0, 2).at[0].set(1)
        loads = jnp.zeros((N_GX,), jnp.int32).at[sigma[0::2]].set(1 + heavy).at[sigma[1::2]].set(1 - heavy)
        ceiling = jnp.cumsum(loads)
        starts = ceiling - loads
        position = jnp.arange(N_GX, dtype=jnp.int32)
        receiver = jnp.sum((ceiling[None, :] <= position[:, None]).astype(jnp.int32), axis=1)
        ordering = jax.random.permutation(keys[2], N_GX)
        owners = receiver[ordering]
        ranks = ordering - starts[owners]
        shuffles = jax.vmap(lambda sub_key: jax.random.permutation(sub_key, cell_total))(jax.random.split(keys[3], N_GX))
        picks = ranks[:, None] * CAP + jnp.arange(CAP, dtype=jnp.int32)[None, :]
        cells_to = shuffles[owners[:, None], picks]
        fills = jax.random.randint(keys[4], (N_GX, cell_total), SLOTS // 4, SLOTS + 1)
        rows_all = jnp.arange(N_GX, dtype=jnp.int32)[:, None]
        fills = fills.at[rows_all, shuffles[:, 2 * CAP:2 * CAP + 1]].set(SLOTS)
        fills = fills.at[rows_all, shuffles[:, :2 * CAP]].set(0)
        owner_table = jnp.broadcast_to(owners[:, None], (N_GX, CAP))
        return (owner_table, cells_to, fills)
    column_keys = jax.random.split(jax.random.fold_in(key, 11), N_GY * N_GZ)
    owners, cells_to, fills = jax.vmap(one_column)(column_keys)
    owners = owners.reshape(N_GY, N_GZ, N_GX, CAP)
    cells_to = cells_to.reshape(N_GY, N_GZ, N_GX, CAP)
    fills = fills.reshape(N_GY, N_GZ, N_GX, CX, CY, CZ)
    return (owners, cells_to, fills)


def draw_mover_owner(key, part):
    owners, cells_to, fills = column_plan(key)
    return owners.transpose(2, 3, 0, 1).reshape(N_GX * CAP, N_GY, N_GZ).astype(jnp.int32)


def draw_mover_cell(key, part):
    owners, cells_to, fills = column_plan(key)
    return cells_to.transpose(2, 3, 0, 1).reshape(N_GX * CAP, N_GY, N_GZ).astype(jnp.int32)


def draw_occupancy(key, part):
    owners, cells_to, fills = column_plan(key)
    return fills.transpose(2, 3, 0, 4, 1, 5).reshape(CX * N_GX, CY * N_GY, CZ * N_GZ).astype(jnp.int32)


def touch_ends(result, own_key, low, high):
    longest = result.shape.index(max(result.shape))
    spots = []
    for shift in (0, 1):
        where = [jax.random.randint(jax.random.fold_in(own_key, axis), (), 0, length) for axis, length in enumerate(result.shape)]
        where[longest] = (where[longest] + shift) % result.shape[longest]
        spots.append(tuple(where))
    return result.at[spots[0]].set(low).at[spots[1]].set(high)


def level_of(rng, dims, pieces, low, top_value):
    gain, own = 1.0, jax.random.fold_in(rng, 6)
    for dim, shards_of in pieces:
        draws = jnp.exp(jax.random.uniform(jax.random.fold_in(own, dim), (shards_of,), jnp.float32, low / len(pieces), top_value / len(pieces)))
        gain = gain * jnp.repeat(draws, dims[dim] // shards_of).reshape([-1 if axis == dim else 1 for axis in range(len(dims))])
    return gain


def gaussian(key, dims, width, limit, cuts=(), held_as=jnp.bfloat16):
    values = width * jax.random.normal(key, dims, jnp.float32)
    if cuts:
        values = values * level_of(key, dims, cuts, -0.22, 0.18)
    return jnp.clip(values, -limit, limit).astype(held_as)


def setup_inputs(seed: int = 0) -> dict:
    splits = jax.random.split(jax.random.key(seed), 9)
    return {
        "positions": jnp.clip(1.0 * jax.random.uniform(splits[0], (3, NX, NY, NZ, SLOTS), jnp.float32) ** level_of(splits[0], (3, NX, NY, NZ, SLOTS), ((1, 4), (2, 4), (3, 2)), -0.2, 0.2), 0.0, 1.0),
        "velocities": gaussian(splits[1], (3, NX, NY, NZ, SLOTS), 1.0, 6.0, ((1, 4), (2, 4), (3, 2)), jnp.float32),
        "occupancy": draw_occupancy(jax.random.fold_in(splits[8], 71), 0),
        "mover_pos": jnp.clip(1.0 * jax.random.uniform(splits[3], (3, MOVERS, N_GY, N_GZ, SLOTS), jnp.float32) ** level_of(splits[3], (3, MOVERS, N_GY, N_GZ, SLOTS), ((1, 4), (2, 4), (3, 2)), -0.2, 0.2), 0.0, 1.0),
        "mover_vel": gaussian(splits[4], (3, MOVERS, N_GY, N_GZ, SLOTS), 1.0, 6.0, ((1, 4), (2, 4), (3, 2)), jnp.float32),
        "mover_count": touch_ends(jax.random.randint(splits[5], (MOVERS, N_GY, N_GZ), 1, SLOTS + 1), jax.random.fold_in(splits[5], 1), 1, SLOTS).astype(jnp.int32),
        "mover_owner": draw_mover_owner(jax.random.fold_in(splits[8], 71), 0),
        "mover_cell": draw_mover_cell(jax.random.fold_in(splits[8], 71), 0),
    }


eps_soft = 0.05
kick_step = 0.02
drift_step = 0.1
far_away = 1000.0

def pair_force(targets, sources, displace):
    separation = sources[:, :, None, :] + displace[:, None, None, None] - targets[:, :, :, None]
    squared = lax.optimization_barrier(jnp.sum(separation * separation, axis=0))
    inside = jnp.maximum(1.0 - squared, 0.0)
    weight = inside * inside / ((squared + eps_soft) * jnp.sqrt(squared + eps_soft))
    return lax.optimization_barrier(jnp.sum(weight[None] * separation, axis=3))

def reference(positions, velocities, occupancy, mover_pos, mover_vel, mover_count, mover_owner, mover_cell):
    plane = CY * CZ
    row_x = (mover_owner * CX + mover_cell // plane).astype(jnp.int32)
    row_y = (jnp.arange(N_GY, dtype=jnp.int32)[None, :, None] * CY + mover_cell // CZ % CY).astype(jnp.int32)
    row_z = (jnp.arange(N_GZ, dtype=jnp.int32)[None, None, :] * CZ + mover_cell % CZ).astype(jnp.int32)
    positions = positions.at[:, row_x, row_y, row_z, :].set(mover_pos)
    velocities = velocities.at[:, row_x, row_y, row_z, :].set(mover_vel)
    occupancy = occupancy.at[row_x, row_y, row_z].set(mover_count)
    live = jnp.arange(SLOTS, dtype=jnp.int32)[None, None, None, :] < occupancy[..., None]
    sources = jnp.where(live[None], positions, far_away)
    padded = jnp.pad(sources, ((0, 0), (1, 1), (1, 1), (1, 1), (0, 0)), mode='wrap')
    cell_total = NX * NY * NZ
    block_size = math.gcd(cell_total, 256)
    block_total = cell_total // block_size
    targets = positions.reshape(3, block_total, block_size, SLOTS).transpose(1, 0, 2, 3)
    force = jnp.zeros((block_total, 3, block_size, SLOTS), jnp.float32)
    for offset_id in range(27):
        step_x = offset_id // 9
        step_y = offset_id // 3 % 3
        step_z = offset_id % 3
        window = padded[:, step_x:step_x + NX, step_y:step_y + NY, step_z:step_z + NZ, :]
        window = window.reshape(3, block_total, block_size, SLOTS).transpose(1, 0, 2, 3)
        displace = jnp.array([step_x - 1, step_y - 1, step_z - 1], jnp.float32)
        force = force + lax.map(lambda paired: pair_force(paired[0], paired[1], displace), (targets, window))
    force = force.transpose(1, 0, 2, 3).reshape(3, NX, NY, NZ, SLOTS)
    new_velocities = jnp.where(live[None], velocities + kick_step * force, 0.0)
    new_positions = jnp.where(live[None], positions + drift_step * new_velocities, 0.0)
    return (new_positions, new_velocities)
```

```python
import functools

import jax
import jax.numpy as jnp
from jax import lax
from jax.experimental import pallas as pl
from jax.experimental.pallas import tpu as pltpu
from jax.sharding import PartitionSpec as P

eps_soft = 0.05
kick_step = 0.02
drift_step = 0.1
far_away = 1000.0

f32, bf16 = jnp.float32, jnp.bfloat16


def offsets(count):
    return sorted({0, 1 % count, count - 1})


def halo_steps():
    steps = [
        (dx, dy, dz)
        for dx in (-1, 0, 1)
        for dy in (-1, 0, 1)
        for dz in (-1, 0, 1)
        if (dx, dy, dz) != (0, 0, 0)
    ]
    return sorted(steps, key=lambda step: -sum(abs(d) for d in step))


def row_index(shape):
    return lax.broadcasted_iota(jnp.int32, shape, len(shape) - 2)


def exchange_kernel(
    axes, dims, leaving, occ_s, count_s, owner_s, cell_s, pos_ref, vel_ref, mpos_ref, mvel_ref,
    halo_ref, velm_ref, line, mov, send, recv, msend, mrecv
):
    nx, ny, nz = axes
    sx, sy, sz = dims
    slots = pos_ref.shape[-1]
    me = [lax.axis_index(name) for name in ("gx", "gy", "gz")]

    def device(step):
        return tuple(lax.rem(m + s, n) for m, s, n in zip(me, step, axes))

    near = sorted(
        {tuple(d % n for d, n in zip(step, axes)) for step in halo_steps()} - {(0, 0, 0)}
    )
    far = [ox for ox in range(nx) if ox not in offsets(nx)]

    def along_line(body, start):
        if nx <= 4:
            for ox in range(start, nx):
                body(ox)
        else:
            lax.fori_loop(start, nx, lambda ox, carry: (body(ox), carry)[1], 0)

    def halo_copy(step):
        source, target = [], []
        for d, size in zip(step, dims):
            if d == 0:
                source.append(pl.ds(1, size))
                target.append(pl.ds(1, size))
            elif d == 1:
                source.append(pl.ds(size, 1))
                target.append(pl.ds(0, 1))
            else:
                source.append(pl.ds(1, 1))
                target.append(pl.ds(size + 1, 1))
        number = (step[0] + 1) * 9 + (step[1] + 1) * 3 + step[2] + 1
        return pltpu.make_async_remote_copy(
            src_ref=halo_ref.at[(*source, pl.ds(0, 3))],
            dst_ref=halo_ref.at[(*target, pl.ds(0, 3))],
            send_sem=send.at[number],
            recv_sem=recv.at[number],
            device_id=device([d % n for d, n in zip(step, axes)]),
            device_id_type=pl.DeviceIdType.MESH,
        )

    def mover_copy(ox):
        return pltpu.make_async_remote_copy(
            src_ref=mov,
            dst_ref=line.at[pl.ds(me[0] * leaving, leaving)],
            send_sem=msend.at[ox],
            recv_sem=mrecv.at[ox],
            device_id=device((ox, 0, 0)),
            device_id_type=pl.DeviceIdType.MESH,
        )

    barrier = pltpu.get_barrier_semaphore()

    def greet(step):
        pl.semaphore_signal(
            barrier, inc=1, device_id=device(step), device_id_type=pl.DeviceIdType.MESH
        )

    for step in near:
        greet(step)
    if nx <= 4:
        for ox in far:
            greet((ox, 0, 0))
    else:
        lax.fori_loop(2, nx - 1, lambda ox, carry: (greet((ox, 0, 0)), carry)[1], 0)

    lane = lax.broadcasted_iota(jnp.int32, (1, slots), 1)
    base = me[0] * (sx * sy * sz)
    for b in range(leaving):
        live = lane < count_s[b]
        rows = [jnp.where(live, mpos_ref[k, b], far_away) for k in range(3)]
        rows += [mvel_ref[k, b] for k in range(3)]
        label = owner_s[b] * (sx * sy * sz) + cell_s[b]
        rows += [jnp.full((1, slots), label, jnp.int32).astype(f32)] * 2
        for k, row in enumerate(rows):
            mov[b, k : k + 1, :] = row
            line[me[0] * leaving + b, k : k + 1, :] = row

    pl.semaphore_wait(barrier, len(near) + len(far))
    along_line(lambda ox: mover_copy(ox).start(), 1)

    sub = row_index((sz, slots))
    lanes = lax.broadcasted_iota(jnp.int32, (sz, slots), 1)
    planes, where = [], []
    for x in range(sx):
        for y in range(sy):
            counts = jnp.zeros((sz, slots), jnp.int32)
            for z in range(sz):
                counts = jnp.where(sub == z, occ_s[x, y, z], counts)
            live = lanes < counts
            planes.append(
                [jnp.where(live, pos_ref[k, x, y], far_away) for k in range(3)]
                + [vel_ref[k, x, y] for k in range(3)]
            )
            where.append((sub + (base + (x * sy + y) * sz)).astype(f32))
    along_line(lambda ox: mover_copy(ox).wait(), 1)

    def merge(b, planes):
        rows = [line[b, pl.ds(k, 1), :] for k in range(7)]
        out = []
        for plane, here in zip(planes, where):
            hit = here == rows[6]
            out.append([jnp.where(hit, row, old) for row, old in zip(rows, plane)])
        return out

    if nx <= 4:
        for b in range(nx * leaving):
            planes = merge(b, planes)
    else:
        planes = lax.fori_loop(0, nx * leaving, merge, planes)

    flat = halo_ref.reshape((sx + 2) * (sy + 2) * (sz + 2) * 8, slots)
    for x in range(sx):
        for y in range(sy):
            first = (((x + 1) * (sy + 2) + y + 1) * (sz + 2) + 1) * 8
            for k in range(3):
                flat[pl.ds(first + k, sz, stride=8), :] = planes[x * sy + y][k]
    for step in halo_steps():
        halo_copy(step).start()
    for x in range(sx):
        for y in range(sy):
            for k in range(3):
                velm_ref[k, x, y] = planes[x * sy + y][3 + k]
    for step in halo_steps():
        halo_copy(step).wait()


def split(value):
    high = value.astype(bf16).astype(f32)
    rest = value - high
    middle = rest.astype(bf16).astype(f32)
    return high, middle, rest - middle


def stack(high, middle, low):
    return jnp.concatenate([high, high, high, middle, middle, low], -2).astype(bf16)


def force_kernel(
    dims, unroll, halo_ref, vel_ref, npos_ref, nvel_ref, left, left2, right, right2, src, src2, total
):
    sx, sy, sz = dims
    hx, hy, hz = (size + 2 for size in dims)
    slots = halo_ref.shape[-1]
    sub = row_index((8, slots))

    def centre(x, y):
        return x - 1 - 0.5 * sx, y - 1 - 0.5 * sy

    def sources(x, y):
        ox, oy = centre(x, y)
        shift = jnp.where(sub == 0, ox, jnp.where(sub == 1, oy, -0.5)).astype(f32)
        out = []
        for z in range(hz):
            extra = jnp.where(sub == 6, 1.0, jnp.where(sub == 7, float(z - 1 - sz // 2), 0.0))
            at = jnp.where(sub < 3, halo_ref[x, y, z] + shift, 0.0)
            high, middle, low = split(at + pltpu.roll(at * at, 3, 0) + extra.astype(f32))
            both = jnp.concatenate([high, middle], 0).astype(bf16)
            out.append((stack(high, middle, low), jnp.concatenate([both, both], 1)))
        return out

    def prepare(x):
        for y in range(1, sy + 1):
            for z, (keys, twice) in enumerate(sources(x, y)):
                left[x, y - 1, z] = keys.T
                src[x, y - 1, z] = twice
        for pair in range(sy // 2):
            low, up = sources(x, 2 * pair), sources(x, 2 * pair + 3)
            for z in range(hz):
                left2[x, pair, z] = jnp.concatenate([low[z][0], up[z][0]], 0).T
                src2[x, pair, z] = jnp.concatenate([low[z][1], up[z][1]], 0)

    def targets(x, pair, z):
        tiles = []
        for y in (2 * pair, 2 * pair + 1):
            ox, oy = centre(x + 1, y + 1)
            shift = jnp.where(sub == 0, ox, jnp.where(sub == 1, oy, -0.5)).astype(f32)
            at = halo_ref[x + 1, y + 1, z + 1]
            tiles.append(jnp.where(at < 0.5 * far_away, at, 0.5) + shift)
        zero = jnp.zeros((48, slots), bf16)
        for e in (-1, 0, 1):
            keys = []
            for at in tiles:
                at = jnp.where(sub < 3, at - jnp.where(sub == 2, float(e), 0.0).astype(f32), 0.0)
                norm = jnp.sum(at * at, axis=0, keepdims=True) + eps_soft
                key = jnp.where(sub < 3, -2.0 * at, jnp.where(sub < 6, 1.0, norm))
                key = jnp.where(sub < 7, key, 0.0)
                high, middle, low = split(key)
                keys.append(
                    jnp.concatenate([high, middle, low, high, middle, high], 0).astype(bf16)
                )
            right[x, pair, z, e + 1] = jnp.concatenate(keys, 1)
            right2[x, pair, z, e + 1] = jnp.concatenate(
                [jnp.concatenate([keys[0], zero], 1), jnp.concatenate([zero, keys[1]], 1)], 0
            )

    def weights(t):
        y = lax.rsqrt(t)
        a = jnp.maximum((1.0 + eps_soft) - t, 0.0) * y
        w = a * a * y
        high = w.astype(bf16)
        return jnp.concatenate([high, (w - high.astype(f32)).astype(bf16)], 0)

    def accumulate(steps, sums):
        lag = 2

        def distances(n):
            return jnp.dot(steps[n][0][...], steps[n][1][...], preferred_element_type=f32)

        queue, ready = [distances(0)], []
        for n in range(len(steps) + lag):
            if n < len(steps):
                if n + 1 < len(steps):
                    queue.append(distances(n + 1))
                ready.append(weights(queue.pop(0)))
            if n >= lag:
                step = steps[n - lag]
                sums[step[3]] = sums[step[3]] + jnp.dot(
                    step[2][...], ready.pop(0), preferred_element_type=f32
                )
        return sums

    def steps_of(x, pair, z, slot):
        steps = []
        for e in range(3):
            for dx in range(3):
                for y in (2 * pair, 2 * pair + 1):
                    steps.append((
                        left.at[x + dx, y, z + e], right.at[x, pair, z, e],
                        src.at[x + dx, y, z + e], 2 * slot,
                    ))
        for e in range(3):
            for dx in range(3):
                steps.append((
                    left2.at[x + dx, pair, z + e], right2.at[x, pair, z, e],
                    src2.at[x + dx, pair, z + e], 2 * slot + 1,
                ))
        return steps

    for x in range(hx):
        prepare(x)
    for x in range(sx):
        for pair in range(sy // 2):
            for z in range(sz):
                targets(x, pair, z)
    for x in range(sx):
        for pair in range(sy // 2):

            def body(i, carry, x=x, pair=pair):
                steps, sums = [], []
                for u in range(unroll):
                    steps += steps_of(x, pair, i * unroll + u, u)
                    sums += [jnp.zeros((16, 2 * slots), f32), jnp.zeros((32, 2 * slots), f32)]
                sums = accumulate(steps, sums)
                for u in range(unroll):
                    one, two = sums[2 * u], sums[2 * u + 1]
                    z = i * unroll + u
                    total[x, pair, 0, z] = one[:, :slots] + two[:16, :slots]
                    total[x, pair, 1, z] = one[:, slots:] + two[16:, slots:]
                return carry

            lax.fori_loop(0, sz // unroll, body, 0)

    flat = halo_ref.reshape(hx * hy * hz * 8, slots)
    for x in range(sx):
        for y in range(sy):
            sums = total.at[x, y // 2, y % 2].reshape(sz * 16, slots)

            def row(r, sums=sums):
                return sums[pl.ds(r, sz, stride=16), :]

            first = (((x + 1) * hy + y + 1) * hz + 1) * 8
            ox, oy = centre(x + 1, y + 1)
            zat = (row_index((sz, slots)) - sz // 2).astype(f32)
            live = None
            for k, shift in enumerate((ox, oy, -0.5)):
                raw = flat[pl.ds(first + k, sz, stride=8), :]
                if k == 0:
                    live = raw < 0.5 * far_away
                high, middle, low = split(raw + shift)
                at, sum_s = high + middle, row(k) + row(8 + k)
                if k == 2:
                    at, sum_s = at + zat, sum_s + row(7)
                force = sum_s - at * row(6)
                vel = jnp.where(live, vel_ref[k, x, y] + kick_step * force, 0.0)
                nvel_ref[k, x, y] = vel
                npos_ref[k, x, y] = jnp.where(live, raw + drift_step * vel, 0.0)


def exchange(occupancy, count, owner, cell, pos, vel, mpos, mvel):
    axes = tuple(lax.axis_size(name) for name in ("gx", "gy", "gz"))
    dims, leaving, slots = pos.shape[1:4], mpos.shape[1], mpos.shape[3]
    padded = tuple(size + 2 for size in dims) + (8, slots)
    vmem = pl.BlockSpec(memory_space=pltpu.VMEM)
    return pl.pallas_call(
        functools.partial(exchange_kernel, axes, dims, leaving),
        out_shape=(pltpu.VMEM(padded, f32), pltpu.VMEM(vel.shape, f32)),
        in_specs=[pl.BlockSpec(memory_space=pltpu.SMEM)] * 4 + [vmem] * 4,
        out_specs=(vmem, vmem),
        scratch_shapes=[
            pltpu.VMEM((axes[0] * leaving, 8, slots), f32),
            pltpu.VMEM((leaving, 8, slots), f32),
            pltpu.SemaphoreType.DMA((27,)),
            pltpu.SemaphoreType.DMA((27,)),
            pltpu.SemaphoreType.DMA((axes[0],)),
            pltpu.SemaphoreType.DMA((axes[0],)),
        ],
        compiler_params=pltpu.CompilerParams(collective_id=0, has_side_effects=True),
        name="exchange",
    )(occupancy, count, owner, cell, pos, vel, mpos, mvel)


def forces(halo, speeds):
    sx, sy, sz = dims = speeds.shape[1:4]
    hx, hz, slots, pairs = sx + 2, sz + 2, speeds.shape[4], sy // 2
    out = jax.ShapeDtypeStruct(speeds.shape, f32)
    vmem = pl.BlockSpec(memory_space=pltpu.VMEM)
    return pl.pallas_call(
        functools.partial(force_kernel, dims, 4 if sz % 4 == 0 else 1),
        out_shape=(out, out),
        in_specs=[vmem] * 2,
        out_specs=(vmem, vmem),
        scratch_shapes=[
            pltpu.VMEM((hx, sy, hz, slots, 48), bf16),
            pltpu.VMEM((hx, pairs, hz, slots, 96), bf16),
            pltpu.VMEM((sx, pairs, sz, 3, 48, 2 * slots), bf16),
            pltpu.VMEM((sx, pairs, sz, 3, 96, 2 * slots), bf16),
            pltpu.VMEM((hx, sy, hz, 16, 2 * slots), bf16),
            pltpu.VMEM((hx, pairs, hz, 32, 2 * slots), bf16),
            pltpu.VMEM((sx, pairs, 2, sz, 16, slots), f32),
        ],
        compiler_params=pltpu.CompilerParams(vmem_limit_bytes=32 * 1024 * 1024),
        name="forces",
    )(halo, speeds)


def per_device(
    positions, velocities, occupancy, mover_pos, mover_vel, mover_count, mover_owner, mover_cell
):
    slots, leaving = positions.shape[4], mover_pos.shape[1]
    halo, speeds = exchange(
        occupancy,
        mover_count.reshape(leaving),
        mover_owner.reshape(leaving),
        mover_cell.reshape(leaving),
        positions,
        velocities,
        mover_pos.reshape(3, leaving, 1, slots),
        mover_vel.reshape(3, leaving, 1, slots),
    )
    return forces(halo, speeds)


def solution(mesh):
    cells = P(None, "gx", "gy", "gz", None)
    labels = P("gx", "gy", "gz")
    return jax.shard_map(
        per_device,
        mesh=mesh,
        in_specs=(cells, cells, labels, cells, cells, labels, labels, labels),
        out_specs=(cells, cells),
        check_vma=False,
    )
```

```python
import functools

import jax
import jax.numpy as jnp
from jax import lax
from jax.experimental import pallas as pl
from jax.experimental.pallas import tpu as pltpu
from jax.sharding import PartitionSpec as P

eps_soft = 0.05
kick_step = 0.02
drift_step = 0.1
far_away = 1000.0

f32, bf16 = jnp.float32, jnp.bfloat16


def offsets(count):
    return sorted({0, 1 % count, count - 1})


def halo_steps():
    steps = [
        (dx, dy, dz)
        for dx in (-1, 0, 1)
        for dy in (-1, 0, 1)
        for dz in (-1, 0, 1)
        if (dx, dy, dz) != (0, 0, 0)
    ]
    return sorted(steps, key=lambda step: -sum(abs(d) for d in step))


def row_index(shape):
    return lax.broadcasted_iota(jnp.int32, shape, len(shape) - 2)


def split(value):
    high = value.astype(bf16).astype(f32)
    rest = value - high
    middle = rest.astype(bf16).astype(f32)
    return high, middle, rest - middle


def stack(high, middle, low):
    return jnp.concatenate([high, high, high, middle, middle, low], -2).astype(bf16)


def centre(dims, x, y):
    return x - 1 - 0.5 * dims[0], y - 1 - 0.5 * dims[1]


def pair_kernel(
    axes, dims, leaving, unroll, occ_h, count_h, owner_h, cell_h, pos_h, vel_h, mpos_h, mvel_h,
    halo_ref, velm_ref, total, occ_s, count_s, owner_s, cell_s, pos_ref, vel_ref, mpos_ref,
    mvel_ref, line, mov, left, left2, right, right2, src, src2, send, recv, msend, mrecv, fetch, known
):
    nx, ny, nz = axes
    sx, sy, sz = dims
    hx, hy, hz = (size + 2 for size in dims)
    slots = pos_ref.shape[-1]
    fetches = [
        pltpu.make_async_copy(there, here, fetch.at[i])
        for i, (there, here) in enumerate([
            (mpos_h, mpos_ref), (mvel_h, mvel_ref), (count_h, count_s), (owner_h, owner_s),
            (cell_h, cell_s), (occ_h, occ_s), (pos_h, pos_ref), (vel_h, vel_ref),
        ])
    ]
    for copy in fetches:
        copy.start()
    me = [lax.axis_index(name) for name in ("gx", "gy", "gz")]

    def device(step):
        return tuple(lax.rem(m + s, n) for m, s, n in zip(me, step, axes))

    def along_line(body, start):
        if nx <= 4:
            for ox in range(start, nx):
                body(ox)
        else:
            lax.fori_loop(start, nx, lambda ox, carry: (body(ox), carry)[1], 0)

    def halo_copy(step):
        source, target = [], []
        for d, size in zip(step, dims):
            if d == 0:
                source.append(pl.ds(1, size))
                target.append(pl.ds(1, size))
            elif d == 1:
                source.append(pl.ds(size, 1))
                target.append(pl.ds(0, 1))
            else:
                source.append(pl.ds(1, 1))
                target.append(pl.ds(size + 1, 1))
        number = (step[0] + 1) * 9 + (step[1] + 1) * 3 + step[2] + 1
        return pltpu.make_async_remote_copy(
            src_ref=halo_ref.at[(*source, pl.ds(0, 3))],
            dst_ref=halo_ref.at[(*target, pl.ds(0, 3))],
            send_sem=send.at[number],
            recv_sem=recv.at[number],
            device_id=device([d % n for d, n in zip(step, axes)]),
            device_id_type=pl.DeviceIdType.MESH,
        )

    def mover_copy(ox, part):
        rows = pl.ds(4 * part, 4)
        return pltpu.make_async_remote_copy(
            src_ref=mov.at[:, rows],
            dst_ref=line.at[pl.ds(me[0] * leaving, leaving), rows],
            send_sem=msend.at[part, ox],
            recv_sem=mrecv.at[part, ox],
            device_id=device((ox, 0, 0)),
            device_id_type=pl.DeviceIdType.MESH,
        )

    tile = row_index((8, slots))

    def sources(x, y, z0, z1):
        ox, oy = centre(dims, x, y)
        shift = jnp.where(tile == 0, ox, jnp.where(tile == 1, oy, -0.5)).astype(f32)
        out = {}
        for z in range(z0, z1):
            extra = jnp.where(tile == 6, 1.0, jnp.where(tile == 7, float(z - 1 - sz // 2), 0.0))
            at = jnp.where(tile < 3, halo_ref[x, y, z] + shift, 0.0)
            high, middle, low = split(at + pltpu.roll(at * at, 3, 0) + extra.astype(f32))
            both = jnp.concatenate([high, middle], 0).astype(bf16)
            out[z] = stack(high, middle, low), jnp.concatenate([both, both], 1)
        return out

    def shared_columns(x, z0, z1):
        for y in range(1, sy + 1):
            for z, (keys, twice) in sources(x, y, z0, z1).items():
                left[x, y - 1, z] = keys.T
                src[x, y - 1, z] = twice

    def split_columns(x):
        for pair in range(sy // 2):
            low, up = sources(x, 2 * pair, 0, hz), sources(x, 2 * pair + 3, 0, hz)
            for z in range(hz):
                left2[x, pair, z] = jnp.concatenate([low[z][0], up[z][0]], 0).T
                src2[x, pair, z] = jnp.concatenate([low[z][1], up[z][1]], 0)

    def targets(x, pair, z):
        tiles = []
        for y in (2 * pair, 2 * pair + 1):
            ox, oy = centre(dims, x + 1, y + 1)
            shift = jnp.where(tile == 0, ox, jnp.where(tile == 1, oy, -0.5)).astype(f32)
            at = halo_ref[x + 1, y + 1, z + 1]
            tiles.append(jnp.where(at < 0.5 * far_away, at, 0.5) + shift)
        zero = jnp.zeros((48, slots), bf16)
        for e in (-1, 0, 1):
            keys = []
            for at in tiles:
                at = jnp.where(tile < 3, at - jnp.where(tile == 2, float(e), 0.0).astype(f32), 0.0)
                norm = jnp.sum(at * at, axis=0, keepdims=True) + eps_soft
                key = jnp.where(tile < 3, -2.0 * at, jnp.where(tile < 6, 1.0, norm))
                key = jnp.where(tile < 7, key, 0.0)
                high, middle, low = split(key)
                keys.append(
                    jnp.concatenate([high, middle, low, high, middle, high], 0).astype(bf16)
                )
            right[x, pair, z, e + 1] = jnp.concatenate(keys, 1)
            right2[x, pair, z, e + 1] = jnp.concatenate(
                [jnp.concatenate([keys[0], zero], 1), jnp.concatenate([zero, keys[1]], 1)], 0
            )

    def weights(t):
        y = lax.rsqrt(t)
        a = jnp.maximum((1.0 + eps_soft) - t, 0.0) * y
        w = a * a * y
        high = w.astype(bf16)
        return jnp.concatenate([high, (w - high.astype(f32)).astype(bf16)], 0)

    def accumulate(steps, sums):
        lag = 2

        def distances(n):
            return jnp.dot(steps[n][0][...], steps[n][1][...], preferred_element_type=f32)

        queue, ready = [distances(0)], []
        for n in range(len(steps) + lag):
            if n < len(steps):
                if n + 1 < len(steps):
                    queue.append(distances(n + 1))
                ready.append(weights(queue.pop(0)))
            if n >= lag:
                step = steps[n - lag]
                sums[step[3]] = sums[step[3]] + jnp.dot(
                    step[2][...], ready.pop(0), preferred_element_type=f32
                )
        return sums

    def steps_of(columns, shared, x, pair, z, slot):
        steps = []
        for e in range(3):
            for dx in columns:
                if shared:
                    for y in (2 * pair, 2 * pair + 1):
                        steps.append((
                            left.at[dx, y, z + e], right.at[x, pair, z, e], src.at[dx, y, z + e], slot
                        ))
                else:
                    steps.append((
                        left2.at[dx, pair, z + e], right2.at[x, pair, z, e],
                        src2.at[dx, pair, z + e], slot,
                    ))
        return steps

    def phase(columns, shared, first):
        for x in range(sx):
            near_x = [dx for dx in columns if x <= dx <= x + 2]
            for pair in range(sy // 2):

                def body(i, carry, x=x, pair=pair, near_x=near_x):
                    steps = []
                    for u in range(unroll):
                        steps += steps_of(near_x, shared, x, pair, i * unroll + u, u)
                    zero = jnp.zeros((16 if shared else 32, 2 * slots), f32)
                    sums = accumulate(steps, [zero] * unroll)
                    for u in range(unroll):
                        z = i * unroll + u
                        for half in range(2):
                            rows = slice(0, 16) if shared else slice(16 * half, 16 * half + 16)
                            part = sums[u][rows, half * slots : (half + 1) * slots]
                            if not first:
                                part = part + total[x, pair, half, z]
                            total[x, pair, half, z] = part
                    return carry

                lax.fori_loop(0, sz // unroll, body, 0)

    def arrive(which):
        for step in halo_steps():
            if which(*step):
                halo_copy(step).wait_recv()

    barrier = pltpu.get_barrier_semaphore()
    ys, zs = offsets(ny)[1:], offsets(nz)[1:]

    def greet(sem, step):
        pl.semaphore_signal(
            sem, inc=1, device_id=device(step), device_id_type=pl.DeviceIdType.MESH
        )

    for oz in zs:
        greet(barrier, (0, 0, oz))
    odd = me[1] % 2
    along_line(lambda ox: greet(barrier, (ox, 0, 0)), 1)

    for copy in fetches[:5]:
        copy.wait()
    lane = lax.broadcasted_iota(jnp.int32, (1, slots), 1)
    base = me[0] * (sx * sy * sz)
    for b in range(leaving):
        live = lane < count_s[b]
        rows = [jnp.where(live, mpos_ref[k, b], far_away) for k in range(3)]
        label = owner_s[b] * (sx * sy * sz) + cell_s[b]
        rows += [jnp.full((1, slots), label, jnp.int32).astype(f32)]
        rows += [mvel_ref[k, b] for k in range(3)]
        for k, row in enumerate(rows):
            mov[b, k : k + 1, :] = row
            line[me[0] * leaving + b, k : k + 1, :] = row

    pl.semaphore_wait(barrier, nx - 1 + len(zs) + odd * len(ys))
    along_line(lambda ox: mover_copy(ox, 0).start(), 1)

    @pl.when(odd == 0)
    def _():
        for oy in ys:
            greet(barrier, (0, oy, 0))

    @pl.when(odd == 1)
    def _():
        for i, oy in enumerate(ys):
            greet(known.at[i], (0, oy, 0))

    for i, oz in enumerate(zs):
        greet(known.at[2 + i], (0, 0, oz))

    for copy in fetches[5:]:
        copy.wait()
    sub = row_index((sz, slots))
    lanes = lax.broadcasted_iota(jnp.int32, (sz, slots), 1)
    planes, where = [], []
    for x in range(sx):
        for y in range(sy):
            counts = jnp.zeros((sz, slots), jnp.int32)
            for z in range(sz):
                counts = jnp.where(sub == z, occ_s[x, y, z], counts)
            live = lanes < counts
            planes.append(
                [jnp.where(live, pos_ref[k, x, y], far_away) for k in range(3)]
            )
            where.append((sub + (base + (x * sy + y) * sz)).astype(f32))
    along_line(lambda ox: mover_copy(ox, 0).wait(), 1)

    def merge(first):
        def one(b, planes):
            label = line[b, pl.ds(3, 1), :]
            rows = [line[b, pl.ds(first + k, 1), :] for k in range(3)]
            return [
                [jnp.where(here == label, row, old) for row, old in zip(rows, plane)]
                for plane, here in zip(planes, where)
            ]

        return one

    def merged(first, planes):
        if nx <= 4:
            for b in range(nx * leaving):
                planes = merge(first)(b, planes)
            return planes
        return lax.fori_loop(0, nx * leaving, merge(first), planes)

    planes = merged(0, planes)

    flat = halo_ref.reshape((sx + 2) * (sy + 2) * (sz + 2) * 8, slots)
    for x in range(sx):
        for y in range(sy):
            first = (((x + 1) * (sy + 2) + y + 1) * (sz + 2) + 1) * 8
            for k in range(3):
                flat[pl.ds(first + k, sz, stride=8), :] = planes[x * sy + y][k]
    assert ny % 2 == 0

    def send_where(which):
        for step in halo_steps():
            if which(*step):
                halo_copy(step).start()

    send_where(lambda dx, dy, dz: abs(dx) + abs(dy) + abs(dz) == 1 and dy == 0)
    for i in range(len(zs)):
        pl.semaphore_wait(known.at[2 + i], 1)
    send_where(lambda dx, dy, dz: dx != 0 and dy == 0 and dz != 0)
    along_line(lambda ox: mover_copy(ox, 1).start(), 1)

    @pl.when(odd == 0)
    def _():
        for i in range(len(ys)):
            pl.semaphore_wait(known.at[i], 1)

    for i, oz in enumerate(zs):
        greet(known.at[4 + i], (0, 0, oz))
    send_where(lambda dx, dy, dz: dx != 0 and dy != 0 and dz == 0)
    send_where(lambda dx, dy, dz: dx == 0 and dy != 0)

    inner = range(1, sx + 1)
    for x in range(sx):
        for pair in range(sy // 2):
            for z in range(sz):
                targets(x, pair, z)
    for x in inner:
        shared_columns(x, 1, sz + 1)
    arrive(lambda dx, dy, dz: dx == 0 and dy == 0)
    for x in inner:
        shared_columns(x, 0, 1)
        shared_columns(x, sz + 1, sz + 2)
    phase(inner, True, True)
    for i in range(len(zs)):
        pl.semaphore_wait(known.at[4 + i], 1)
    send_where(lambda dx, dy, dz: dx != 0 and dy != 0 and dz != 0)
    arrive(lambda dx, dy, dz: dx != 0 and dy == 0)
    outer = (0, sx + 1)
    for x in outer:
        shared_columns(x, 0, hz)
    phase(outer, True, False)
    arrive(lambda dx, dy, dz: dy != 0)
    for x in range(hx):
        split_columns(x)
    phase(range(hx), False, False)
    along_line(lambda ox: mover_copy(ox, 1).wait(), 1)
    speeds = merged(4, [[vel_ref[k, x, y] for k in range(3)] for x in range(sx) for y in range(sy)])
    for x in range(sx):
        for y in range(sy):
            for k in range(3):
                velm_ref[k, x, y] = speeds[x * sy + y][k]
    for step in halo_steps():
        halo_copy(step).wait_send()


def kick_kernel(dims, halo_ref, vel_ref, total, npos_ref, nvel_ref):
    sx, sy, sz = dims
    hx, hy, hz = (size + 2 for size in dims)
    slots = halo_ref.shape[-1]
    flat = halo_ref.reshape(hx * hy * hz * 8, slots)
    for x in range(sx):
        for y in range(sy):
            sums = total.at[x, y // 2, y % 2].reshape(sz * 16, slots)

            def row(r, sums=sums):
                return sums[pl.ds(r, sz, stride=16), :]

            first = (((x + 1) * hy + y + 1) * hz + 1) * 8
            ox, oy = centre(dims, x + 1, y + 1)
            zat = (row_index((sz, slots)) - sz // 2).astype(f32)
            live = None
            for k, shift in enumerate((ox, oy, -0.5)):
                raw = flat[pl.ds(first + k, sz, stride=8), :]
                if k == 0:
                    live = raw < 0.5 * far_away
                high, middle, low = split(raw + shift)
                at, sum_s = high + middle, row(k) + row(8 + k)
                if k == 2:
                    at, sum_s = at + zat, sum_s + row(7)
                force = sum_s - at * row(6)
                vel = jnp.where(live, vel_ref[k, x, y] + kick_step * force, 0.0)
                nvel_ref[k, x, y] = vel
                npos_ref[k, x, y] = jnp.where(live, raw + drift_step * vel, 0.0)


def pair_sums(occupancy, count, owner, cell, pos, vel, mpos, mvel):
    axes = tuple(lax.axis_size(name) for name in ("gx", "gy", "gz"))
    sx, sy, sz = dims = pos.shape[1:4]
    leaving, slots = mpos.shape[1], mpos.shape[3]
    hx, hy, hz = padded = tuple(size + 2 for size in dims)
    pairs, wide = sy // 2, 2 * slots
    unroll = 4 if sz % 4 == 0 else 1
    vmem = pl.BlockSpec(memory_space=pltpu.VMEM)
    ints = (occupancy, count, owner, cell)
    return pl.pallas_call(
        functools.partial(pair_kernel, axes, dims, leaving, unroll),
        out_shape=(
            pltpu.VMEM((*padded, 8, slots), f32),
            pltpu.VMEM(vel.shape, f32),
            pltpu.VMEM((sx, pairs, 2, sz, 16, slots), f32),
        ),
        in_specs=[pl.BlockSpec(memory_space=pl.ANY)] * 8,
        out_specs=(vmem, vmem, vmem),
        scratch_shapes=[
            *[pltpu.SMEM(value.shape, jnp.int32) for value in ints],
            *[pltpu.VMEM(value.shape, f32) for value in (pos, vel, mpos, mvel)],
            pltpu.VMEM((axes[0] * leaving, 8, slots), f32),
            pltpu.VMEM((leaving, 8, slots), f32),
            pltpu.VMEM((hx, sy, hz, slots, 48), bf16),
            pltpu.VMEM((hx, pairs, hz, slots, 96), bf16),
            pltpu.VMEM((sx, pairs, sz, 3, 48, wide), bf16),
            pltpu.VMEM((sx, pairs, sz, 3, 96, wide), bf16),
            pltpu.VMEM((hx, sy, hz, 16, wide), bf16),
            pltpu.VMEM((hx, pairs, hz, 32, wide), bf16),
            pltpu.SemaphoreType.DMA((27,)),
            pltpu.SemaphoreType.DMA((27,)),
            pltpu.SemaphoreType.DMA((2, axes[0])),
            pltpu.SemaphoreType.DMA((2, axes[0])),
            pltpu.SemaphoreType.DMA((8,)),
            pltpu.SemaphoreType.REGULAR((6,)),
        ],
        compiler_params=pltpu.CompilerParams(collective_id=0, has_side_effects=True),
        name="pairs",
    )(*ints, pos, vel, mpos, mvel)


def kick(halo, speeds, sums):
    out = jax.ShapeDtypeStruct(speeds.shape, f32)
    vmem = pl.BlockSpec(memory_space=pltpu.VMEM)
    return pl.pallas_call(
        functools.partial(kick_kernel, speeds.shape[1:4]),
        out_shape=(out, out),
        in_specs=[vmem] * 3,
        out_specs=(vmem, vmem),
        compiler_params=pltpu.CompilerParams(vmem_limit_bytes=16 * 1024 * 1024),
        name="kick",
    )(halo, speeds, sums)


def per_device(
    positions, velocities, occupancy, mover_pos, mover_vel, mover_count, mover_owner, mover_cell
):
    slots, leaving = positions.shape[4], mover_pos.shape[1]
    halo, speeds, sums = pair_sums(
        occupancy,
        mover_count.reshape(leaving),
        mover_owner.reshape(leaving),
        mover_cell.reshape(leaving),
        positions,
        velocities,
        mover_pos.reshape(3, leaving, 1, slots),
        mover_vel.reshape(3, leaving, 1, slots),
    )
    return kick(halo, speeds, sums)


def solution(mesh):
    cells = P(None, "gx", "gy", "gz", None)
    labels = P("gx", "gy", "gz")
    return jax.shard_map(
        per_device,
        mesh=mesh,
        in_specs=(cells, cells, labels, cells, cells, labels, labels, labels),
        out_specs=(cells, cells),
        check_vma=False,
    )
```

```python
import functools

import jax
import jax.numpy as jnp
from jax import lax
from jax.experimental import pallas as pl
from jax.experimental.pallas import tpu as pltpu
from jax.sharding import PartitionSpec as P

eps_soft = 0.05
kick_step = 0.02
drift_step = 0.1
far_away = 1000.0

f32, bf16 = jnp.float32, jnp.bfloat16


def offsets(count):
    return sorted({0, 1 % count, count - 1})


def halo_steps():
    steps = [
        (dx, dy, dz)
        for dx in (-1, 0, 1)
        for dy in (-1, 0, 1)
        for dz in (-1, 0, 1)
        if (dx, dy, dz) != (0, 0, 0)
    ]
    return sorted(steps, key=lambda step: -sum(abs(d) for d in step))


def row_index(shape):
    return lax.broadcasted_iota(jnp.int32, shape, len(shape) - 2)


def split(value):
    high = value.astype(bf16).astype(f32)
    rest = value - high
    middle = rest.astype(bf16).astype(f32)
    return high, middle, rest - middle


def stack(high, middle, low):
    return jnp.concatenate([high, high, high, middle, middle, low], -2).astype(bf16)


def centre(dims, x, y):
    return x - 1 - 0.5 * dims[0], y - 1 - 0.5 * dims[1]


def pair_kernel(
    axes, dims, leaving, unroll, occ_h, count_h, owner_h, cell_h, pos_h, vel_h, mpos_h, mvel_h,
    halo_ref, velm_ref, total, occ_s, count_s, owner_s, cell_s, pos_ref, vel_ref, mpos_ref,
    mvel_ref, line, mov, left, left2, right, right2, src, src2, send, recv, msend, mrecv, fetch, known
):
    nx, ny, nz = axes
    sx, sy, sz = dims
    hx, hy, hz = (size + 2 for size in dims)
    slots = pos_ref.shape[-1]
    fetches = [
        pltpu.make_async_copy(there, here, fetch.at[i])
        for i, (there, here) in enumerate([
            (mpos_h, mpos_ref), (mvel_h, mvel_ref), (count_h, count_s), (owner_h, owner_s),
            (cell_h, cell_s), (occ_h, occ_s), (pos_h, pos_ref), (vel_h, vel_ref),
        ])
    ]
    for copy in fetches:
        copy.start()
    me = [lax.axis_index(name) for name in ("gx", "gy", "gz")]

    def device(step):
        return tuple(lax.rem(m + s, n) for m, s, n in zip(me, step, axes))

    def along_line(body, start):
        if nx <= 4:
            for ox in range(start, nx):
                body(ox)
        else:
            lax.fori_loop(start, nx, lambda ox, carry: (body(ox), carry)[1], 0)

    def halo_copy(step):
        source, target = [], []
        for d, size in zip(step, dims):
            if d == 0:
                source.append(pl.ds(1, size))
                target.append(pl.ds(1, size))
            elif d == 1:
                source.append(pl.ds(size, 1))
                target.append(pl.ds(0, 1))
            else:
                source.append(pl.ds(1, 1))
                target.append(pl.ds(size + 1, 1))
        number = (step[0] + 1) * 9 + (step[1] + 1) * 3 + step[2] + 1
        return pltpu.make_async_remote_copy(
            src_ref=halo_ref.at[(*source, pl.ds(0, 3))],
            dst_ref=halo_ref.at[(*target, pl.ds(0, 3))],
            send_sem=send.at[number],
            recv_sem=recv.at[number],
            device_id=device([d % n for d, n in zip(step, axes)]),
            device_id_type=pl.DeviceIdType.MESH,
        )

    def mover_copy(ox, part):
        rows = pl.ds(4 * part, 4)
        return pltpu.make_async_remote_copy(
            src_ref=mov.at[:, rows],
            dst_ref=line.at[pl.ds(me[0] * leaving, leaving), rows],
            send_sem=msend.at[part, ox],
            recv_sem=mrecv.at[part, ox],
            device_id=device((ox, 0, 0)),
            device_id_type=pl.DeviceIdType.MESH,
        )

    tile = row_index((8, slots))

    def sources(x, y, z0, z1):
        ox, oy = centre(dims, x, y)
        shift = jnp.where(tile == 0, ox, jnp.where(tile == 1, oy, -0.5)).astype(f32)
        out = {}
        for z in range(z0, z1):
            extra = jnp.where(tile == 6, 1.0, jnp.where(tile == 7, float(z - 1 - sz // 2), 0.0))
            at = jnp.where(tile < 3, halo_ref[x, y, z] + shift, 0.0)
            high, middle, low = split(at + pltpu.roll(at * at, 3, 0) + extra.astype(f32))
            both = jnp.concatenate([high, middle], 0).astype(bf16)
            out[z] = stack(high, middle, low), jnp.concatenate([both, both], 1)
        return out

    def shared_columns(x, z0, z1):
        for y in range(1, sy + 1):
            for z, (keys, twice) in sources(x, y, z0, z1).items():
                left[x, y - 1, z] = keys.T
                src[x, y - 1, z] = twice

    def split_columns(x):
        for pair in range(sy // 2):
            low, up = sources(x, 2 * pair, 0, hz), sources(x, 2 * pair + 3, 0, hz)
            for z in range(hz):
                left2[x, pair, z] = jnp.concatenate([low[z][0], up[z][0]], 0).T
                src2[x, pair, z] = jnp.concatenate([low[z][1], up[z][1]], 0)

    def targets(x, pair, z):
        tiles = []
        for y in (2 * pair, 2 * pair + 1):
            ox, oy = centre(dims, x + 1, y + 1)
            shift = jnp.where(tile == 0, ox, jnp.where(tile == 1, oy, -0.5)).astype(f32)
            at = halo_ref[x + 1, y + 1, z + 1]
            tiles.append(jnp.where(at < 0.5 * far_away, at, 0.5) + shift)
        zero = jnp.zeros((48, slots), bf16)
        for e in (-1, 0, 1):
            keys = []
            for at in tiles:
                at = jnp.where(tile < 3, at - jnp.where(tile == 2, float(e), 0.0).astype(f32), 0.0)
                norm = jnp.sum(at * at, axis=0, keepdims=True) + eps_soft
                key = jnp.where(tile < 3, -2.0 * at, jnp.where(tile < 6, 1.0, norm))
                key = jnp.where(tile < 7, key, 0.0)
                high, middle, low = split(key)
                keys.append(
                    jnp.concatenate([high, middle, low, high, middle, high], 0).astype(bf16)
                )
            right[x, pair, z, e + 1] = jnp.concatenate(keys, 1)
            right2[x, pair, z, e + 1] = jnp.concatenate(
                [jnp.concatenate([keys[0], zero], 1), jnp.concatenate([zero, keys[1]], 1)], 0
            )

    def weights(t):
        y = lax.rsqrt(t)
        a = jnp.maximum((1.0 + eps_soft) - t, 0.0) * y
        w = a * a * y
        high = w.astype(bf16)
        return jnp.concatenate([high, (w - high.astype(f32)).astype(bf16)], 0)

    def accumulate(steps, sums):
        lag = 2

        def distances(n):
            return jnp.dot(steps[n][0][...], steps[n][1][...], preferred_element_type=f32)

        queue, ready = [distances(0)], []
        for n in range(len(steps) + lag):
            if n < len(steps):
                if n + 1 < len(steps):
                    queue.append(distances(n + 1))
                ready.append(weights(queue.pop(0)))
            if n >= lag:
                step = steps[n - lag]
                sums[step[3]] = sums[step[3]] + jnp.dot(
                    step[2][...], ready.pop(0), preferred_element_type=f32
                )
        return sums

    def steps_of(columns, shared, levels, x, pair, z, slot):
        steps = []
        for e in levels:
            for dx in columns:
                if shared:
                    for y in (2 * pair, 2 * pair + 1):
                        steps.append((
                            left.at[dx, y, z + e], right.at[x, pair, z, e], src.at[dx, y, z + e], slot
                        ))
                else:
                    steps.append((
                        left2.at[dx, pair, z + e], right2.at[x, pair, z, e],
                        src2.at[dx, pair, z + e], slot,
                    ))
        return steps

    def phase(columns, shared, levels=(0, 1, 2), first=False, unroll=unroll):
        for x in range(sx):
            near_x = [dx for dx in columns if x <= dx <= x + 2]
            for pair in range(sy // 2):

                def body(i, carry, x=x, pair=pair, near_x=near_x):
                    steps = []
                    for u in range(unroll):
                        steps += steps_of(near_x, shared, levels, x, pair, i * unroll + u, u)
                    zero = jnp.zeros((16 if shared else 32, 2 * slots), f32)
                    sums = accumulate(steps, [zero] * unroll)
                    for u in range(unroll):
                        z = i * unroll + u
                        for half in range(2):
                            rows = slice(0, 16) if shared else slice(16 * half, 16 * half + 16)
                            part = sums[u][rows, half * slots : (half + 1) * slots]
                            if not first:
                                part = part + total[x, pair, half, z]
                            total[x, pair, half, z] = part
                    return carry

                lax.fori_loop(0, sz // unroll, body, 0)

    def arrive(which):
        for step in halo_steps():
            if which(*step):
                halo_copy(step).wait_recv()

    barrier = pltpu.get_barrier_semaphore()
    ys, zs = offsets(ny)[1:], offsets(nz)[1:]

    def greet(sem, step):
        pl.semaphore_signal(
            sem, inc=1, device_id=device(step), device_id_type=pl.DeviceIdType.MESH
        )

    for oz in zs:
        greet(barrier, (0, 0, oz))
    odd = me[1] % 2

    @pl.when(odd == 0)
    def _():
        for oy in ys:
            greet(barrier, (0, oy, 0))

    along_line(lambda ox: greet(barrier, (ox, 0, 0)), 1)

    for copy in fetches[:5]:
        copy.wait()
    lane = lax.broadcasted_iota(jnp.int32, (1, slots), 1)
    base = me[0] * (sx * sy * sz)
    for b in range(leaving):
        live = lane < count_s[b]
        rows = [jnp.where(live, mpos_ref[k, b], far_away) for k in range(3)]
        label = owner_s[b] * (sx * sy * sz) + cell_s[b]
        rows += [jnp.full((1, slots), label, jnp.int32).astype(f32)]
        rows += [mvel_ref[k, b] for k in range(3)]
        for k, row in enumerate(rows):
            mov[b, k : k + 1, :] = row
            line[me[0] * leaving + b, k : k + 1, :] = row

    pl.semaphore_wait(barrier, nx - 1 + len(zs) + odd * len(ys))
    along_line(lambda ox: mover_copy(ox, 0).start(), 1)

    @pl.when(odd == 1)
    def _():
        for i, oy in enumerate(ys):
            greet(known.at[i], (0, oy, 0))

    for i, oz in enumerate(zs):
        greet(known.at[2 + i], (0, 0, oz))

    for copy in fetches[5:]:
        copy.wait()
    sub = row_index((sz, slots))
    lanes = lax.broadcasted_iota(jnp.int32, (sz, slots), 1)
    planes, where = [], []
    for x in range(sx):
        for y in range(sy):
            counts = jnp.zeros((sz, slots), jnp.int32)
            for z in range(sz):
                counts = jnp.where(sub == z, occ_s[x, y, z], counts)
            live = lanes < counts
            planes.append(
                [jnp.where(live, pos_ref[k, x, y], far_away) for k in range(3)]
            )
            where.append((sub + (base + (x * sy + y) * sz)).astype(f32))
    along_line(lambda ox: mover_copy(ox, 0).wait(), 1)

    def merge(first):
        def one(b, planes):
            label = line[b, pl.ds(3, 1), :]
            rows = [line[b, pl.ds(first + k, 1), :] for k in range(3)]
            return [
                [jnp.where(here == label, row, old) for row, old in zip(rows, plane)]
                for plane, here in zip(planes, where)
            ]

        return one

    def merged(first, planes):
        if nx <= 4:
            for b in range(nx * leaving):
                planes = merge(first)(b, planes)
            return planes
        return lax.fori_loop(0, nx * leaving, merge(first), planes)

    planes = merged(0, planes)

    flat = halo_ref.reshape((sx + 2) * (sy + 2) * (sz + 2) * 8, slots)
    for x in range(sx):
        for y in range(sy):
            first = (((x + 1) * (sy + 2) + y + 1) * (sz + 2) + 1) * 8
            for k in range(3):
                flat[pl.ds(first + k, sz, stride=8), :] = planes[x * sy + y][k]
    assert ny % 2 == 0

    def send_where(which):
        for step in halo_steps():
            if which(*step):
                halo_copy(step).start()

    send_where(lambda dx, dy, dz: abs(dx) + abs(dy) + abs(dz) == 1 and dy == 0)
    for i in range(len(zs)):
        pl.semaphore_wait(known.at[2 + i], 1)
    send_where(lambda dx, dy, dz: dx != 0 and dy == 0 and dz != 0)
    along_line(lambda ox: mover_copy(ox, 1).start(), 1)

    inner, outer = range(1, sx + 1), (0, sx + 1)
    for x in range(sx):
        for pair in range(sy // 2):
            for z in range(sz):
                targets(x, pair, z)
    for x in inner:
        shared_columns(x, 1, sz + 1)
    @pl.when(odd == 0)
    def _():
        for i, oy in enumerate(ys):
            pl.semaphore_wait(known.at[i], 1)
        for i, oy in enumerate(ys):
            greet(known.at[i], (0, oy, 0))

    phase(inner, True, (1,), True, sz)

    @pl.when(odd == 1)
    def _():
        for i in range(len(ys)):
            pl.semaphore_wait(known.at[i], 1)

    for i, oz in enumerate(zs):
        greet(known.at[4 + i], (0, 0, oz))
    send_where(lambda dx, dy, dz: dx != 0 and dy != 0 and dz == 0)
    send_where(lambda dx, dy, dz: dx == 0 and dy != 0)
    along_line(lambda ox: mover_copy(ox, 1).wait(), 1)
    speeds = merged(4, [[vel_ref[k, x, y] for k in range(3)] for x in range(sx) for y in range(sy)])
    for x in range(sx):
        for y in range(sy):
            for k in range(3):
                velm_ref[k, x, y] = speeds[x * sy + y][k]
    arrive(lambda dx, dy, dz: dx == 0 and dy == 0)
    for x in inner:
        shared_columns(x, 0, 1)
        shared_columns(x, sz + 1, sz + 2)
    for i in range(len(zs)):
        pl.semaphore_wait(known.at[4 + i], 1)
    send_where(lambda dx, dy, dz: dx != 0 and dy != 0 and dz != 0)
    phase(inner, True, (0, 2), False, sz)
    arrive(lambda dx, dy, dz: dx != 0 and dy == 0)
    for x in outer:
        shared_columns(x, 0, hz)
    phase(outer, True)
    arrive(lambda dx, dy, dz: dy != 0)
    for x in range(hx):
        split_columns(x)
    phase(range(hx), False)
    for step in halo_steps():
        halo_copy(step).wait_send()


def kick_kernel(dims, halo_ref, vel_ref, total, npos_ref, nvel_ref):
    sx, sy, sz = dims
    hx, hy, hz = (size + 2 for size in dims)
    slots = halo_ref.shape[-1]
    flat = halo_ref.reshape(hx * hy * hz * 8, slots)
    for x in range(sx):
        for y in range(sy):
            sums = total.at[x, y // 2, y % 2].reshape(sz * 16, slots)

            def row(r, sums=sums):
                return sums[pl.ds(r, sz, stride=16), :]

            first = (((x + 1) * hy + y + 1) * hz + 1) * 8
            ox, oy = centre(dims, x + 1, y + 1)
            zat = (row_index((sz, slots)) - sz // 2).astype(f32)
            live = None
            for k, shift in enumerate((ox, oy, -0.5)):
                raw = flat[pl.ds(first + k, sz, stride=8), :]
                if k == 0:
                    live = raw < 0.5 * far_away
                high, middle, low = split(raw + shift)
                at, sum_s = high + middle, row(k) + row(8 + k)
                if k == 2:
                    at, sum_s = at + zat, sum_s + row(7)
                force = sum_s - at * row(6)
                vel = jnp.where(live, vel_ref[k, x, y] + kick_step * force, 0.0)
                nvel_ref[k, x, y] = vel
                npos_ref[k, x, y] = jnp.where(live, raw + drift_step * vel, 0.0)


def pair_sums(occupancy, count, owner, cell, pos, vel, mpos, mvel):
    axes = tuple(lax.axis_size(name) for name in ("gx", "gy", "gz"))
    sx, sy, sz = dims = pos.shape[1:4]
    leaving, slots = mpos.shape[1], mpos.shape[3]
    hx, hy, hz = padded = tuple(size + 2 for size in dims)
    pairs, wide = sy // 2, 2 * slots
    unroll = 4 if sz % 4 == 0 else 1
    vmem = pl.BlockSpec(memory_space=pltpu.VMEM)
    ints = (occupancy, count, owner, cell)
    return pl.pallas_call(
        functools.partial(pair_kernel, axes, dims, leaving, unroll),
        out_shape=(
            pltpu.VMEM((*padded, 8, slots), f32),
            pltpu.VMEM(vel.shape, f32),
            pltpu.VMEM((sx, pairs, 2, sz, 16, slots), f32),
        ),
        in_specs=[pl.BlockSpec(memory_space=pl.ANY)] * 8,
        out_specs=(vmem, vmem, vmem),
        scratch_shapes=[
            *[pltpu.SMEM(value.shape, jnp.int32) for value in ints],
            *[pltpu.VMEM(value.shape, f32) for value in (pos, vel, mpos, mvel)],
            pltpu.VMEM((axes[0] * leaving, 8, slots), f32),
            pltpu.VMEM((leaving, 8, slots), f32),
            pltpu.VMEM((hx, sy, hz, slots, 48), bf16),
            pltpu.VMEM((hx, pairs, hz, slots, 96), bf16),
            pltpu.VMEM((sx, pairs, sz, 3, 48, wide), bf16),
            pltpu.VMEM((sx, pairs, sz, 3, 96, wide), bf16),
            pltpu.VMEM((hx, sy, hz, 16, wide), bf16),
            pltpu.VMEM((hx, pairs, hz, 32, wide), bf16),
            pltpu.SemaphoreType.DMA((27,)),
            pltpu.SemaphoreType.DMA((27,)),
            pltpu.SemaphoreType.DMA((2, axes[0])),
            pltpu.SemaphoreType.DMA((2, axes[0])),
            pltpu.SemaphoreType.DMA((8,)),
            pltpu.SemaphoreType.REGULAR((6,)),
        ],
        compiler_params=pltpu.CompilerParams(collective_id=0, has_side_effects=True),
        name="pairs",
    )(*ints, pos, vel, mpos, mvel)


def kick(halo, speeds, sums):
    out = jax.ShapeDtypeStruct(speeds.shape, f32)
    vmem = pl.BlockSpec(memory_space=pltpu.VMEM)
    return pl.pallas_call(
        functools.partial(kick_kernel, speeds.shape[1:4]),
        out_shape=(out, out),
        in_specs=[vmem] * 3,
        out_specs=(vmem, vmem),
        compiler_params=pltpu.CompilerParams(vmem_limit_bytes=16 * 1024 * 1024),
        name="kick",
    )(halo, speeds, sums)


def per_device(
    positions, velocities, occupancy, mover_pos, mover_vel, mover_count, mover_owner, mover_cell
):
    slots, leaving = positions.shape[4], mover_pos.shape[1]
    halo, speeds, sums = pair_sums(
        occupancy,
        mover_count.reshape(leaving),
        mover_owner.reshape(leaving),
        mover_cell.reshape(leaving),
        positions,
        velocities,
        mover_pos.reshape(3, leaving, 1, slots),
        mover_vel.reshape(3, leaving, 1, slots),
    )
    return kick(halo, speeds, sums)


def solution(mesh):
    cells = P(None, "gx", "gy", "gz", None)
    labels = P("gx", "gy", "gz")
    return jax.shard_map(
        per_device,
        mesh=mesh,
        in_specs=(cells, cells, labels, cells, cells, labels, labels, labels),
        out_specs=(cells, cells),
        check_vma=False,
    )
```

```python
import functools

import jax
import jax.numpy as jnp
from jax import lax
from jax.experimental import pallas as pl
from jax.experimental.pallas import tpu as pltpu
from jax.sharding import PartitionSpec as P

eps_soft = 0.05
kick_step = 0.02
drift_step = 0.1
far_away = 1000.0

f32, bf16 = jnp.float32, jnp.bfloat16


def offsets(count):
    return sorted({0, 1 % count, count - 1})


def halo_steps():
    steps = [
        (dx, dy, dz)
        for dx in (-1, 0, 1)
        for dy in (-1, 0, 1)
        for dz in (-1, 0, 1)
        if (dx, dy, dz) != (0, 0, 0)
    ]
    return sorted(steps, key=lambda step: -sum(abs(d) for d in step))


def row_index(shape):
    return lax.broadcasted_iota(jnp.int32, shape, len(shape) - 2)


def split(value):
    high = value.astype(bf16).astype(f32)
    rest = value - high
    middle = rest.astype(bf16).astype(f32)
    return high, middle, rest - middle


def stack(high, middle, low):
    return jnp.concatenate([high, high, high, middle, middle, low], -2).astype(bf16)


def centre(dims, x, y):
    return x - 1 - 0.5 * dims[0], y - 1 - 0.5 * dims[1]


def pair_kernel(
    axes, dims, leaving, unroll, occ_h, count_h, owner_h, cell_h, pos_h, vel_h, mpos_h, mvel_h,
    halo_ref, velm_ref, total, occ_s, count_s, owner_s, cell_s, pos_ref, vel_ref, mpos_ref,
    mvel_ref, line, mov, left, left2, right, right2, src, src2, send, recv, msend, mrecv, fetch, known, ahead,
    behind
):
    nx, ny, nz = axes
    sx, sy, sz = dims
    hx, hy, hz = (size + 2 for size in dims)
    slots = pos_ref.shape[-1]
    fetches = [
        pltpu.make_async_copy(there, here, fetch.at[i])
        for i, (there, here) in enumerate([
            (mpos_h, mpos_ref), (mvel_h, mvel_ref), (count_h, count_s), (owner_h, owner_s),
            (cell_h, cell_s), (occ_h, occ_s), (pos_h, pos_ref), (vel_h, vel_ref),
        ])
    ]
    for copy in fetches:
        copy.start()
    me = [lax.axis_index(name) for name in ("gx", "gy", "gz")]

    def device(step):
        return tuple(lax.rem(m + s, n) for m, s, n in zip(me, step, axes))

    def along_line(body, start):
        if nx <= 4:
            for ox in range(start, nx):
                body(ox)
        else:
            lax.fori_loop(start, nx, lambda ox, carry: (body(ox), carry)[1], 0)

    def halo_copy(step):
        source, target = [], []
        for d, size in zip(step, dims):
            if d == 0:
                source.append(pl.ds(1, size))
                target.append(pl.ds(1, size))
            elif d == 1:
                source.append(pl.ds(size, 1))
                target.append(pl.ds(0, 1))
            else:
                source.append(pl.ds(1, 1))
                target.append(pl.ds(size + 1, 1))
        number = (step[0] + 1) * 9 + (step[1] + 1) * 3 + step[2] + 1
        return pltpu.make_async_remote_copy(
            src_ref=halo_ref.at[(*source, pl.ds(0, 3))],
            dst_ref=halo_ref.at[(*target, pl.ds(0, 3))],
            send_sem=send.at[number],
            recv_sem=recv.at[number],
            device_id=device([d % n for d, n in zip(step, axes)]),
            device_id_type=pl.DeviceIdType.MESH,
        )

    def mover_copy(ox, part):
        rows = pl.ds(4 * part, 4)
        return pltpu.make_async_remote_copy(
            src_ref=mov.at[:, rows],
            dst_ref=line.at[pl.ds(me[0] * leaving, leaving), rows],
            send_sem=msend.at[part, ox],
            recv_sem=mrecv.at[part, ox],
            device_id=device((ox, 0, 0)),
            device_id_type=pl.DeviceIdType.MESH,
        )

    tile = row_index((8, slots))

    def sources(x, y, z0, z1):
        ox, oy = centre(dims, x, y)
        shift = jnp.where(tile == 0, ox, jnp.where(tile == 1, oy, -0.5)).astype(f32)
        out = {}
        for z in range(z0, z1):
            extra = jnp.where(tile == 6, 1.0, jnp.where(tile == 7, float(z - 1 - sz // 2), 0.0))
            at = jnp.where(tile < 3, halo_ref[x, y, z] + shift, 0.0)
            high, middle, low = split(at + pltpu.roll(at * at, 3, 0) + extra.astype(f32))
            both = jnp.concatenate([high, middle], 0).astype(bf16)
            out[z] = stack(high, middle, low), jnp.concatenate([both, both], 1)
        return out

    def shared_columns(x, z0, z1):
        for y in range(1, sy + 1):
            for z, (keys, twice) in sources(x, y, z0, z1).items():
                left[x, y - 1, z] = keys.T
                src[x, y - 1, z] = twice

    def split_columns(x):
        for pair in range(sy // 2):
            low, up = sources(x, 2 * pair, 0, hz), sources(x, 2 * pair + 3, 0, hz)
            for z in range(hz):
                left2[x, pair, z] = jnp.concatenate([low[z][0], up[z][0]], 0).T
                src2[x, pair, z] = jnp.concatenate([low[z][1], up[z][1]], 0)

    def targets(x, pair, z):
        tiles = []
        for y in (2 * pair, 2 * pair + 1):
            ox, oy = centre(dims, x + 1, y + 1)
            shift = jnp.where(tile == 0, ox, jnp.where(tile == 1, oy, -0.5)).astype(f32)
            at = halo_ref[x + 1, y + 1, z + 1]
            tiles.append(jnp.where(at < 0.5 * far_away, at, 0.5) + shift)
        zero = jnp.zeros((48, slots), bf16)
        for e in (-1, 0, 1):
            keys = []
            for at in tiles:
                at = jnp.where(tile < 3, at - jnp.where(tile == 2, float(e), 0.0).astype(f32), 0.0)
                norm = jnp.sum(at * at, axis=0, keepdims=True) + eps_soft
                key = jnp.where(tile < 3, -2.0 * at, jnp.where(tile < 6, 1.0, norm))
                key = jnp.where(tile < 7, key, 0.0)
                high, middle, low = split(key)
                keys.append(
                    jnp.concatenate([high, middle, low, high, middle, high], 0).astype(bf16)
                )
            right[x, pair, z, e + 1] = jnp.concatenate(keys, 1)
            right2[x, pair, z, e + 1] = jnp.concatenate(
                [jnp.concatenate([keys[0], zero], 1), jnp.concatenate([zero, keys[1]], 1)], 0
            )

    def weights(t):
        y = lax.rsqrt(t)
        a = jnp.maximum((1.0 + eps_soft) - t, 0.0) * y
        w = a * a * y
        high = w.astype(bf16)
        return jnp.concatenate([high, (w - high.astype(f32)).astype(bf16)], 0)

    def accumulate(steps, sums):
        lag = 2

        def distances(n):
            return jnp.dot(steps[n][0][...], steps[n][1][...], preferred_element_type=f32)

        queue, ready = [distances(0)], []
        for n in range(len(steps) + lag):
            if n < len(steps):
                if n + 1 < len(steps):
                    queue.append(distances(n + 1))
                ready.append(weights(queue.pop(0)))
            if n >= lag:
                step = steps[n - lag]
                sums[step[3]] = sums[step[3]] + jnp.dot(
                    step[2][...], ready.pop(0), preferred_element_type=f32
                )
        return sums

    def steps_of(columns, shared, levels, x, pair, z, slot):
        steps = []
        for e in levels:
            for dx in columns:
                if shared:
                    for y in (2 * pair, 2 * pair + 1):
                        steps.append((
                            left.at[dx, y, z + e], right.at[x, pair, z, e], src.at[dx, y, z + e], slot
                        ))
                else:
                    steps.append((
                        left2.at[dx, pair, z + e], right2.at[x, pair, z, e],
                        src2.at[dx, pair, z + e], slot,
                    ))
        return steps

    def add(x, pair, z, value, shared, first=False):
        for half in range(2):
            rows = slice(0, 16) if shared else slice(16 * half, 16 * half + 16)
            part = value[rows, half * slots : (half + 1) * slots]
            if not first:
                part = part + total[x, pair, half, z]
            total[x, pair, half, z] = part

    def product(step):
        return jnp.dot(step[0][...], step[1][...], preferred_element_type=f32)

    def gather(step, weight):
        return jnp.dot(step[2][...], weight, preferred_element_type=f32)

    def phase(columns, shared, levels=(0, 1, 2), first=False, unroll=unroll):
        rounds, lag = sz // unroll, 2
        zero = jnp.zeros((16 if shared else 32, 2 * slots), f32)
        for x in range(sx):
            near_x = [dx for dx in columns if x <= dx <= x + 2]
            for pair in range(sy // 2):

                def group(i, x=x, pair=pair, near_x=near_x):
                    steps = []
                    for u in range(unroll):
                        steps += steps_of(near_x, shared, levels, x, pair, i * unroll + u, u)
                    return steps

                if rounds == 1:
                    sums = accumulate(group(0), [zero] * unroll)
                    for u in range(unroll):
                        add(x, pair, u, sums[u], shared, first)
                    continue

                ahead[...] = product(group(0)[0])
                for k in range(lag):
                    behind[k] = jnp.zeros(behind.shape[1:], bf16)

                def body(i, carry, x=x, pair=pair, group=group):
                    steps = group(i)
                    following = group(lax.rem(i + 1, rounds))[0]
                    before = group(lax.rem(i + rounds - 1, rounds))[-lag:]
                    sums, late = [zero] * unroll, zero
                    now, ready = ahead[...], []
                    for n in range(len(steps)):
                        then = product(steps[n + 1] if n + 1 < len(steps) else following)
                        ready.append(weights(now))
                        now = then
                        if n < lag:
                            late = late + gather(before[n], behind[n])
                        else:
                            step = steps[n - lag]
                            sums[step[3]] = sums[step[3]] + gather(step, ready.pop(0))
                    for k in range(lag):
                        behind[k] = ready[k]
                    ahead[...] = now
                    for u in range(unroll):
                        add(x, pair, i * unroll + u, sums[u], shared)
                    add(x, pair, lax.rem(i * unroll + sz - 1, sz), late, shared)
                    return carry

                lax.fori_loop(0, rounds, body, 0)
                late = zero
                for k, step in enumerate(group(rounds - 1)[-lag:]):
                    late = late + gather(step, behind[k])
                add(x, pair, sz - 1, late, shared)

    def arrive(which):
        for step in halo_steps():
            if which(*step):
                halo_copy(step).wait_recv()

    barrier = pltpu.get_barrier_semaphore()
    ys, zs = offsets(ny)[1:], offsets(nz)[1:]

    def greet(sem, step):
        pl.semaphore_signal(
            sem, inc=1, device_id=device(step), device_id_type=pl.DeviceIdType.MESH
        )

    for oz in zs:
        greet(barrier, (0, 0, oz))
    odd = me[1] % 2

    @pl.when(odd == 0)
    def _():
        for oy in ys:
            greet(barrier, (0, oy, 0))

    along_line(lambda ox: greet(barrier, (ox, 0, 0)), 1)

    for copy in fetches[:5]:
        copy.wait()
    lane = lax.broadcasted_iota(jnp.int32, (1, slots), 1)
    base = me[0] * (sx * sy * sz)
    for b in range(leaving):
        live = lane < count_s[b]
        rows = [jnp.where(live, mpos_ref[k, b], far_away) for k in range(3)]
        label = owner_s[b] * (sx * sy * sz) + cell_s[b]
        rows += [jnp.full((1, slots), label, jnp.int32).astype(f32)]
        rows += [mvel_ref[k, b] for k in range(3)]
        for k, row in enumerate(rows):
            mov[b, k : k + 1, :] = row
            line[me[0] * leaving + b, k : k + 1, :] = row

    pl.semaphore_wait(barrier, nx - 1 + len(zs) + odd * len(ys))
    along_line(lambda ox: mover_copy(ox, 0).start(), 1)

    @pl.when(odd == 1)
    def _():
        for i, oy in enumerate(ys):
            greet(known.at[i], (0, oy, 0))

    for i, oz in enumerate(zs):
        greet(known.at[2 + i], (0, 0, oz))

    for copy in fetches[5:]:
        copy.wait()
    sub = row_index((sz, slots))
    lanes = lax.broadcasted_iota(jnp.int32, (sz, slots), 1)
    planes, where = [], []
    for x in range(sx):
        for y in range(sy):
            counts = jnp.zeros((sz, slots), jnp.int32)
            for z in range(sz):
                counts = jnp.where(sub == z, occ_s[x, y, z], counts)
            live = lanes < counts
            planes.append(
                [jnp.where(live, pos_ref[k, x, y], far_away) for k in range(3)]
            )
            where.append((sub + (base + (x * sy + y) * sz)).astype(f32))
    along_line(lambda ox: mover_copy(ox, 0).wait(), 1)

    def merge(first):
        def one(b, planes):
            label = line[b, pl.ds(3, 1), :]
            rows = [line[b, pl.ds(first + k, 1), :] for k in range(3)]
            return [
                [jnp.where(here == label, row, old) for row, old in zip(rows, plane)]
                for plane, here in zip(planes, where)
            ]

        return one

    def merged(first, planes):
        if nx <= 4:
            for b in range(nx * leaving):
                planes = merge(first)(b, planes)
            return planes
        return lax.fori_loop(0, nx * leaving, merge(first), planes)

    planes = merged(0, planes)

    flat = halo_ref.reshape((sx + 2) * (sy + 2) * (sz + 2) * 8, slots)
    for x in range(sx):
        for y in range(sy):
            first = (((x + 1) * (sy + 2) + y + 1) * (sz + 2) + 1) * 8
            for k in range(3):
                flat[pl.ds(first + k, sz, stride=8), :] = planes[x * sy + y][k]
    assert ny % 2 == 0

    def send_where(which):
        for step in halo_steps():
            if which(*step):
                halo_copy(step).start()

    send_where(lambda dx, dy, dz: abs(dx) + abs(dy) + abs(dz) == 1 and dy == 0)
    for i in range(len(zs)):
        pl.semaphore_wait(known.at[2 + i], 1)
    send_where(lambda dx, dy, dz: dx != 0 and dy == 0 and dz != 0)
    along_line(lambda ox: mover_copy(ox, 1).start(), 1)

    inner, outer = range(1, sx + 1), (0, sx + 1)
    for x in range(sx):
        for pair in range(sy // 2):
            for z in range(sz):
                targets(x, pair, z)
    for x in inner:
        shared_columns(x, 1, sz + 1)
    @pl.when(odd == 0)
    def _():
        for i, oy in enumerate(ys):
            pl.semaphore_wait(known.at[i], 1)
        for i, oy in enumerate(ys):
            greet(known.at[i], (0, oy, 0))

    phase(inner, True, (1,), True, sz)

    @pl.when(odd == 1)
    def _():
        for i in range(len(ys)):
            pl.semaphore_wait(known.at[i], 1)

    for i, oz in enumerate(zs):
        greet(known.at[4 + i], (0, 0, oz))
    send_where(lambda dx, dy, dz: dx != 0 and dy != 0 and dz == 0)
    send_where(lambda dx, dy, dz: dx == 0 and dy != 0)
    along_line(lambda ox: mover_copy(ox, 1).wait(), 1)
    speeds = merged(4, [[vel_ref[k, x, y] for k in range(3)] for x in range(sx) for y in range(sy)])
    for x in range(sx):
        for y in range(sy):
            for k in range(3):
                velm_ref[k, x, y] = speeds[x * sy + y][k]
    arrive(lambda dx, dy, dz: dx == 0 and dy == 0)
    for x in inner:
        shared_columns(x, 0, 1)
        shared_columns(x, sz + 1, sz + 2)
    for i in range(len(zs)):
        pl.semaphore_wait(known.at[4 + i], 1)
    send_where(lambda dx, dy, dz: dx != 0 and dy != 0 and dz != 0)
    phase(inner, True, (0, 2), False, sz)
    arrive(lambda dx, dy, dz: dx != 0 and dy == 0)
    for x in outer:
        shared_columns(x, 0, hz)
    phase(outer, True)
    arrive(lambda dx, dy, dz: dy != 0)
    for x in range(hx):
        split_columns(x)
    phase(range(hx), False)
    for step in halo_steps():
        halo_copy(step).wait_send()


def kick_kernel(dims, halo_ref, vel_ref, total, npos_ref, nvel_ref):
    sx, sy, sz = dims
    hx, hy, hz = (size + 2 for size in dims)
    slots = halo_ref.shape[-1]
    flat = halo_ref.reshape(hx * hy * hz * 8, slots)
    for x in range(sx):
        for y in range(sy):
            sums = total.at[x, y // 2, y % 2].reshape(sz * 16, slots)

            def row(r, sums=sums):
                return sums[pl.ds(r, sz, stride=16), :]

            first = (((x + 1) * hy + y + 1) * hz + 1) * 8
            ox, oy = centre(dims, x + 1, y + 1)
            zat = (row_index((sz, slots)) - sz // 2).astype(f32)
            live = None
            for k, shift in enumerate((ox, oy, -0.5)):
                raw = flat[pl.ds(first + k, sz, stride=8), :]
                if k == 0:
                    live = raw < 0.5 * far_away
                high, middle, low = split(raw + shift)
                at, sum_s = high + middle, row(k) + row(8 + k)
                if k == 2:
                    at, sum_s = at + zat, sum_s + row(7)
                force = sum_s - at * row(6)
                vel = jnp.where(live, vel_ref[k, x, y] + kick_step * force, 0.0)
                nvel_ref[k, x, y] = vel
                npos_ref[k, x, y] = jnp.where(live, raw + drift_step * vel, 0.0)


def pair_sums(occupancy, count, owner, cell, pos, vel, mpos, mvel):
    axes = tuple(lax.axis_size(name) for name in ("gx", "gy", "gz"))
    sx, sy, sz = dims = pos.shape[1:4]
    leaving, slots = mpos.shape[1], mpos.shape[3]
    hx, hy, hz = padded = tuple(size + 2 for size in dims)
    pairs, wide = sy // 2, 2 * slots
    unroll = 4 if sz % 4 == 0 else 1
    vmem = pl.BlockSpec(memory_space=pltpu.VMEM)
    ints = (occupancy, count, owner, cell)
    return pl.pallas_call(
        functools.partial(pair_kernel, axes, dims, leaving, unroll),
        out_shape=(
            pltpu.VMEM((*padded, 8, slots), f32),
            pltpu.VMEM(vel.shape, f32),
            pltpu.VMEM((sx, pairs, 2, sz, 16, slots), f32),
        ),
        in_specs=[pl.BlockSpec(memory_space=pl.ANY)] * 8,
        out_specs=(vmem, vmem, vmem),
        scratch_shapes=[
            *[pltpu.SMEM(value.shape, jnp.int32) for value in ints],
            *[pltpu.VMEM(value.shape, f32) for value in (pos, vel, mpos, mvel)],
            pltpu.VMEM((axes[0] * leaving, 8, slots), f32),
            pltpu.VMEM((leaving, 8, slots), f32),
            pltpu.VMEM((hx, sy, hz, slots, 48), bf16),
            pltpu.VMEM((hx, pairs, hz, slots, 96), bf16),
            pltpu.VMEM((sx, pairs, sz, 3, 48, wide), bf16),
            pltpu.VMEM((sx, pairs, sz, 3, 96, wide), bf16),
            pltpu.VMEM((hx, sy, hz, 16, wide), bf16),
            pltpu.VMEM((hx, pairs, hz, 32, wide), bf16),
            pltpu.SemaphoreType.DMA((27,)),
            pltpu.SemaphoreType.DMA((27,)),
            pltpu.SemaphoreType.DMA((2, axes[0])),
            pltpu.SemaphoreType.DMA((2, axes[0])),
            pltpu.SemaphoreType.DMA((8,)),
            pltpu.SemaphoreType.REGULAR((6,)),
            pltpu.VMEM((slots, wide), f32),
            pltpu.VMEM((2, 2 * slots, wide), bf16),
        ],
        compiler_params=pltpu.CompilerParams(
            collective_id=0,
            has_side_effects=True,
        ),
        name="pairs",
    )(*ints, pos, vel, mpos, mvel)


def kick(halo, speeds, sums):
    out = jax.ShapeDtypeStruct(speeds.shape, f32)
    vmem = pl.BlockSpec(memory_space=pltpu.VMEM)
    return pl.pallas_call(
        functools.partial(kick_kernel, speeds.shape[1:4]),
        out_shape=(out, out),
        in_specs=[vmem] * 3,
        out_specs=(vmem, vmem),
        compiler_params=pltpu.CompilerParams(vmem_limit_bytes=16 * 1024 * 1024),
        name="kick",
    )(halo, speeds, sums)


def per_device(
    positions, velocities, occupancy, mover_pos, mover_vel, mover_count, mover_owner, mover_cell
):
    slots, leaving = positions.shape[4], mover_pos.shape[1]
    halo, speeds, sums = pair_sums(
        occupancy,
        mover_count.reshape(leaving),
        mover_owner.reshape(leaving),
        mover_cell.reshape(leaving),
        positions,
        velocities,
        mover_pos.reshape(3, leaving, 1, slots),
        mover_vel.reshape(3, leaving, 1, slots),
    )
    return kick(halo, speeds, sums)


def solution(mesh):
    cells = P(None, "gx", "gy", "gz", None)
    labels = P("gx", "gy", "gz")
    return jax.shard_map(
        per_device,
        mesh=mesh,
        in_specs=(cells, cells, labels, cells, cells, labels, labels, labels),
        out_specs=(cells, cells),
        check_vma=False,
    )
```

```python
import functools

import jax
import jax.numpy as jnp
from jax import lax
from jax.experimental import pallas as pl
from jax.experimental.pallas import tpu as pltpu
from jax.sharding import PartitionSpec as P

eps_soft = 0.05
kick_step = 0.02
drift_step = 0.1
far_away = 1000.0

f32, bf16 = jnp.float32, jnp.bfloat16


def offsets(count):
    return sorted({0, 1 % count, count - 1})


def halo_steps():
    steps = [
        (dx, dy, dz)
        for dx in (-1, 0, 1)
        for dy in (-1, 0, 1)
        for dz in (-1, 0, 1)
        if (dx, dy, dz) != (0, 0, 0)
    ]
    return sorted(steps, key=lambda step: -sum(abs(d) for d in step))


def row_index(shape):
    return lax.broadcasted_iota(jnp.int32, shape, len(shape) - 2)


def split(value):
    high = value.astype(bf16).astype(f32)
    rest = value - high
    middle = rest.astype(bf16).astype(f32)
    return high, middle, rest - middle


def stack(high, middle, low):
    return jnp.concatenate([high, high, high, middle, middle, low], -2).astype(bf16)


def centre(dims, x, y):
    return x - 1 - 0.5 * dims[0], y - 1 - 0.5 * dims[1]


def pair_kernel(
    axes, dims, leaving, unroll, occ_h, count_h, owner_h, cell_h, pos_h, vel_h, mpos_h, mvel_h,
    halo_ref, velm_ref, total, occ_s, count_s, owner_s, cell_s, pos_ref, vel_ref, mpos_ref,
    mvel_ref, line, mov, left, left2, right, right2, src, src2, send, recv, msend, mrecv, fetch, known, ahead,
    behind
):
    nx, ny, nz = axes
    sx, sy, sz = dims
    hx, hy, hz = (size + 2 for size in dims)
    slots = pos_ref.shape[-1]
    fetches = [
        pltpu.make_async_copy(there, here, fetch.at[i])
        for i, (there, here) in enumerate([
            (mpos_h, mpos_ref), (mvel_h, mvel_ref), (count_h, count_s), (owner_h, owner_s),
            (cell_h, cell_s), (occ_h, occ_s), (pos_h, pos_ref), (vel_h, vel_ref),
        ])
    ]
    for copy in fetches:
        copy.start()
    me = [lax.axis_index(name) for name in ("gx", "gy", "gz")]

    def device(step):
        return tuple(lax.rem(m + s, n) for m, s, n in zip(me, step, axes))

    def along_line(body, start):
        if nx <= 4:
            for ox in range(start, nx):
                body(ox)
        else:
            lax.fori_loop(start, nx, lambda ox, carry: (body(ox), carry)[1], 0)

    def halo_copy(step):
        source, target = [], []
        for d, size in zip(step, dims):
            if d == 0:
                source.append(pl.ds(1, size))
                target.append(pl.ds(1, size))
            elif d == 1:
                source.append(pl.ds(size, 1))
                target.append(pl.ds(0, 1))
            else:
                source.append(pl.ds(1, 1))
                target.append(pl.ds(size + 1, 1))
        number = (step[0] + 1) * 9 + (step[1] + 1) * 3 + step[2] + 1
        return pltpu.make_async_remote_copy(
            src_ref=halo_ref.at[(*source, pl.ds(0, 3))],
            dst_ref=halo_ref.at[(*target, pl.ds(0, 3))],
            send_sem=send.at[number],
            recv_sem=recv.at[number],
            device_id=device([d % n for d, n in zip(step, axes)]),
            device_id_type=pl.DeviceIdType.MESH,
        )

    def mover_copy(ox, part):
        rows = pl.ds(4 * part, 4)
        return pltpu.make_async_remote_copy(
            src_ref=mov.at[:, rows],
            dst_ref=line.at[pl.ds(me[0] * leaving, leaving), rows],
            send_sem=msend.at[part, ox],
            recv_sem=mrecv.at[part, ox],
            device_id=device((ox, 0, 0)),
            device_id_type=pl.DeviceIdType.MESH,
        )

    tile = row_index((8, slots))

    def sources(x, y, z0, z1):
        ox, oy = centre(dims, x, y)
        shift = jnp.where(tile == 0, ox, jnp.where(tile == 1, oy, -0.5)).astype(f32)
        out = {}
        for z in range(z0, z1):
            extra = jnp.where(tile == 6, 1.0, jnp.where(tile == 7, float(z - 1 - sz // 2), 0.0))
            at = jnp.where(tile < 3, halo_ref[x, y, z] + shift, 0.0)
            high, middle, low = split(at + pltpu.roll(at * at, 3, 0) + extra.astype(f32))
            both = jnp.concatenate([high, middle], 0).astype(bf16)
            out[z] = stack(high, middle, low), jnp.concatenate([both, both], 1)
        return out

    def shared_columns(x, z0, z1):
        for y in range(1, sy + 1):
            for z, (keys, twice) in sources(x, y, z0, z1).items():
                left[x, y - 1, z] = keys.T
                src[x, y - 1, z] = twice

    def split_columns(x):
        for pair in range(sy // 2):
            low, up = sources(x, 2 * pair, 0, hz), sources(x, 2 * pair + 3, 0, hz)
            for z in range(hz):
                left2[x, pair, z] = jnp.concatenate([low[z][0], up[z][0]], 0).T
                src2[x, pair, z] = jnp.concatenate([low[z][1], up[z][1]], 0)

    def targets(x, pair, z):
        tiles = []
        for y in (2 * pair, 2 * pair + 1):
            ox, oy = centre(dims, x + 1, y + 1)
            shift = jnp.where(tile == 0, ox, jnp.where(tile == 1, oy, -0.5)).astype(f32)
            at = halo_ref[x + 1, y + 1, z + 1]
            tiles.append(jnp.where(at < 0.5 * far_away, at, 0.5) + shift)
        zero = jnp.zeros((48, slots), bf16)
        for e in (-1, 0, 1):
            keys = []
            for at in tiles:
                at = jnp.where(tile < 3, at - jnp.where(tile == 2, float(e), 0.0).astype(f32), 0.0)
                norm = jnp.sum(at * at, axis=0, keepdims=True) + eps_soft
                key = jnp.where(tile < 3, -2.0 * at, jnp.where(tile < 6, 1.0, norm))
                key = jnp.where(tile < 7, key, 0.0)
                high, middle, low = split(key)
                keys.append(
                    jnp.concatenate([high, middle, low, high, middle, high], 0).astype(bf16)
                )
            right[x, pair, z, e + 1] = jnp.concatenate(keys, 1)
            right2[x, pair, z, e + 1] = jnp.concatenate(
                [jnp.concatenate([keys[0], zero], 1), jnp.concatenate([zero, keys[1]], 1)], 0
            )

    def weights(t):
        y = lax.rsqrt(t)
        a = jnp.maximum((1.0 + eps_soft) - t, 0.0) * y
        w = a * a * y
        high = w.astype(bf16)
        return jnp.concatenate([high, (w - high.astype(f32)).astype(bf16)], 0)

    def accumulate(steps, sums):
        lag = 2

        def distances(n):
            return jnp.dot(steps[n][0][...], steps[n][1][...], preferred_element_type=f32)

        queue, ready = [distances(0)], []
        for n in range(len(steps) + lag):
            if n < len(steps):
                if n + 1 < len(steps):
                    queue.append(distances(n + 1))
                ready.append(weights(queue.pop(0)))
            if n >= lag:
                step = steps[n - lag]
                sums[step[3]] = sums[step[3]] + jnp.dot(
                    step[2][...], ready.pop(0), preferred_element_type=f32
                )
        return sums

    def steps_of(columns, shared, levels, x, pair, z, slot):
        steps = []
        for e in levels:
            for dx in columns:
                if shared:
                    for y in (2 * pair, 2 * pair + 1):
                        steps.append((
                            left.at[dx, y, z + e], right.at[x, pair, z, e], src.at[dx, y, z + e], slot
                        ))
                else:
                    steps.append((
                        left2.at[dx, pair, z + e], right2.at[x, pair, z, e],
                        src2.at[dx, pair, z + e], slot,
                    ))
        return steps

    def add(x, pair, z, value, shared, first=False):
        for half in range(2):
            rows = slice(0, 16) if shared else slice(16 * half, 16 * half + 16)
            part = value[rows, half * slots : (half + 1) * slots]
            if not first:
                part = part + total[x, pair, half, z]
            total[x, pair, half, z] = part

    def product(step):
        return jnp.dot(step[0][...], step[1][...], preferred_element_type=f32)

    def gather(step, weight):
        return jnp.dot(step[2][...], weight, preferred_element_type=f32)

    def phase(columns, shared, levels=(0, 1, 2), first=False, unroll=unroll):
        rounds, lag = sz // unroll, 2
        zero = jnp.zeros((16 if shared else 32, 2 * slots), f32)
        for x in range(sx):
            near_x = [dx for dx in columns if x <= dx <= x + 2]
            for pair in range(sy // 2):

                def group(i, x=x, pair=pair, near_x=near_x):
                    steps = []
                    for u in range(unroll):
                        steps += steps_of(near_x, shared, levels, x, pair, i * unroll + u, u)
                    return steps

                if rounds == 1:
                    sums = accumulate(group(0), [zero] * unroll)
                    for u in range(unroll):
                        add(x, pair, u, sums[u], shared, first)
                    continue

                ahead[...] = product(group(0)[0])
                for k in range(lag):
                    behind[k] = jnp.zeros(behind.shape[1:], bf16)

                def body(i, carry, x=x, pair=pair, group=group):
                    steps = group(i)
                    following = group(lax.rem(i + 1, rounds))[0]
                    before = group(lax.rem(i + rounds - 1, rounds))[-lag:]
                    sums, late = [zero] * unroll, zero
                    now, ready = ahead[...], []
                    for n in range(len(steps)):
                        then = product(steps[n + 1] if n + 1 < len(steps) else following)
                        ready.append(weights(now))
                        now = then
                        if n < lag:
                            late = late + gather(before[n], behind[n])
                        else:
                            step = steps[n - lag]
                            sums[step[3]] = sums[step[3]] + gather(step, ready.pop(0))
                    for k in range(lag):
                        behind[k] = ready[k]
                    ahead[...] = now
                    for u in range(unroll):
                        add(x, pair, i * unroll + u, sums[u], shared)
                    add(x, pair, lax.rem(i * unroll + sz - 1, sz), late, shared)
                    return carry

                lax.fori_loop(0, rounds, body, 0)
                late = zero
                for k, step in enumerate(group(rounds - 1)[-lag:]):
                    late = late + gather(step, behind[k])
                add(x, pair, sz - 1, late, shared)

    def arrive(which):
        for step in halo_steps():
            if which(*step):
                halo_copy(step).wait_recv()

    barrier = pltpu.get_barrier_semaphore()
    ys, zs = offsets(ny)[1:], offsets(nz)[1:]

    def greet(sem, step):
        pl.semaphore_signal(
            sem, inc=1, device_id=device(step), device_id_type=pl.DeviceIdType.MESH
        )

    for oz in zs:
        greet(barrier, (0, 0, oz))
    odd = me[1] % 2

    @pl.when(odd == 0)
    def _():
        for oy in ys:
            greet(barrier, (0, oy, 0))

    along_line(lambda ox: greet(barrier, (ox, 0, 0)), 1)

    for copy in fetches[:5]:
        copy.wait()
    lane = lax.broadcasted_iota(jnp.int32, (1, slots), 1)
    base = me[0] * (sx * sy * sz)
    for b in range(leaving):
        live = lane < count_s[b]
        rows = [jnp.where(live, mpos_ref[k, b], far_away) for k in range(3)]
        label = owner_s[b] * (sx * sy * sz) + cell_s[b]
        rows += [jnp.full((1, slots), label, jnp.int32).astype(f32)]
        rows += [mvel_ref[k, b] for k in range(3)]
        for k, row in enumerate(rows):
            mov[b, k : k + 1, :] = row
            line[me[0] * leaving + b, k : k + 1, :] = row

    pl.semaphore_wait(barrier, nx - 1 + len(zs) + odd * len(ys))
    along_line(lambda ox: mover_copy(ox, 0).start(), 1)

    @pl.when(odd == 1)
    def _():
        for i, oy in enumerate(ys):
            greet(known.at[i], (0, oy, 0))

    for i, oz in enumerate(zs):
        greet(known.at[2 + i], (0, 0, oz))

    for copy in fetches[5:]:
        copy.wait()
    sub = row_index((sz, slots))
    lanes = lax.broadcasted_iota(jnp.int32, (sz, slots), 1)
    planes, where = [], []
    for x in range(sx):
        for y in range(sy):
            counts = jnp.zeros((sz, slots), jnp.int32)
            for z in range(sz):
                counts = jnp.where(sub == z, occ_s[x, y, z], counts)
            live = lanes < counts
            planes.append(
                [jnp.where(live, pos_ref[k, x, y], far_away) for k in range(3)]
            )
            where.append((sub + (base + (x * sy + y) * sz)).astype(f32))
    along_line(lambda ox: mover_copy(ox, 0).wait_recv(), 1)

    def merge(first):
        def one(b, planes):
            label = line[b, pl.ds(3, 1), :]
            rows = [line[b, pl.ds(first + k, 1), :] for k in range(3)]
            return [
                [jnp.where(here == label, row, old) for row, old in zip(rows, plane)]
                for plane, here in zip(planes, where)
            ]

        return one

    def merged(first, planes):
        if nx <= 4:
            for b in range(nx * leaving):
                planes = merge(first)(b, planes)
            return planes
        return lax.fori_loop(0, nx * leaving, merge(first), planes)

    planes = merged(0, planes)

    flat = halo_ref.reshape((sx + 2) * (sy + 2) * (sz + 2) * 8, slots)
    for x in range(sx):
        for y in range(sy):
            first = (((x + 1) * (sy + 2) + y + 1) * (sz + 2) + 1) * 8
            for k in range(3):
                flat[pl.ds(first + k, sz, stride=8), :] = planes[x * sy + y][k]
    assert ny % 2 == 0

    def send_where(which):
        for step in halo_steps():
            if which(*step):
                halo_copy(step).start()

    send_where(lambda dx, dy, dz: abs(dx) + abs(dy) + abs(dz) == 1 and dy == 0)
    for i in range(len(zs)):
        pl.semaphore_wait(known.at[2 + i], 1)
    send_where(lambda dx, dy, dz: dx != 0 and dy == 0 and dz != 0)
    along_line(lambda ox: mover_copy(ox, 1).start(), 1)

    inner, outer = range(1, sx + 1), (0, sx + 1)
    for x in range(sx):
        for pair in range(sy // 2):
            for z in range(sz):
                targets(x, pair, z)
    for x in inner:
        shared_columns(x, 1, sz + 1)
    @pl.when(odd == 0)
    def _():
        for i, oy in enumerate(ys):
            pl.semaphore_wait(known.at[i], 1)
        for i, oy in enumerate(ys):
            greet(known.at[i], (0, oy, 0))

    @pl.when(odd == 1)
    def _():
        for i in range(len(ys)):
            pl.semaphore_wait(known.at[i], 1)

    for i, oz in enumerate(zs):
        greet(known.at[4 + i], (0, 0, oz))
    send_where(lambda dx, dy, dz: dx != 0 and dy != 0 and dz == 0)
    send_where(lambda dx, dy, dz: dx == 0 and dy != 0)
    phase(inner, True, (1,), True, sz)

    for i in range(len(zs)):
        pl.semaphore_wait(known.at[4 + i], 1)
    send_where(lambda dx, dy, dz: dx != 0 and dy != 0 and dz != 0)
    arrive(lambda dx, dy, dz: dx == 0 and dy == 0)
    for x in inner:
        shared_columns(x, 0, 1)
        shared_columns(x, sz + 1, sz + 2)
    phase(inner, True, (0, 2), False, sz)
    arrive(lambda dx, dy, dz: dx != 0 and dy == 0)
    for x in outer:
        shared_columns(x, 0, hz)
    phase(outer, True)
    along_line(lambda ox: mover_copy(ox, 1).wait(), 1)
    speeds = merged(4, [[vel_ref[k, x, y] for k in range(3)] for x in range(sx) for y in range(sy)])
    for x in range(sx):
        for y in range(sy):
            for k in range(3):
                velm_ref[k, x, y] = speeds[x * sy + y][k]
    arrive(lambda dx, dy, dz: dy != 0)
    for x in range(hx):
        split_columns(x)
    phase(range(hx), False)
    along_line(lambda ox: mover_copy(ox, 0).wait_send(), 1)
    for step in halo_steps():
        halo_copy(step).wait_send()


def kick_kernel(dims, halo_ref, vel_ref, total, npos_ref, nvel_ref):
    sx, sy, sz = dims
    hx, hy, hz = (size + 2 for size in dims)
    slots = halo_ref.shape[-1]
    flat = halo_ref.reshape(hx * hy * hz * 8, slots)
    for x in range(sx):
        for y in range(sy):
            sums = total.at[x, y // 2, y % 2].reshape(sz * 16, slots)

            def row(r, sums=sums):
                return sums[pl.ds(r, sz, stride=16), :]

            first = (((x + 1) * hy + y + 1) * hz + 1) * 8
            ox, oy = centre(dims, x + 1, y + 1)
            zat = (row_index((sz, slots)) - sz // 2).astype(f32)
            live = None
            for k, shift in enumerate((ox, oy, -0.5)):
                raw = flat[pl.ds(first + k, sz, stride=8), :]
                if k == 0:
                    live = raw < 0.5 * far_away
                high, middle, low = split(raw + shift)
                at, sum_s = high + middle, row(k) + row(8 + k)
                if k == 2:
                    at, sum_s = at + zat, sum_s + row(7)
                force = sum_s - at * row(6)
                vel = jnp.where(live, vel_ref[k, x, y] + kick_step * force, 0.0)
                nvel_ref[k, x, y] = vel
                npos_ref[k, x, y] = jnp.where(live, raw + drift_step * vel, 0.0)


def pair_sums(occupancy, count, owner, cell, pos, vel, mpos, mvel):
    axes = tuple(lax.axis_size(name) for name in ("gx", "gy", "gz"))
    sx, sy, sz = dims = pos.shape[1:4]
    leaving, slots = mpos.shape[1], mpos.shape[3]
    hx, hy, hz = padded = tuple(size + 2 for size in dims)
    pairs, wide = sy // 2, 2 * slots
    unroll = 4 if sz % 4 == 0 else 1
    vmem = pl.BlockSpec(memory_space=pltpu.VMEM)
    ints = (occupancy, count, owner, cell)
    return pl.pallas_call(
        functools.partial(pair_kernel, axes, dims, leaving, unroll),
        out_shape=(
            pltpu.VMEM((*padded, 8, slots), f32),
            pltpu.VMEM(vel.shape, f32),
            pltpu.VMEM((sx, pairs, 2, sz, 16, slots), f32),
        ),
        in_specs=[pl.BlockSpec(memory_space=pl.ANY)] * 8,
        out_specs=(vmem, vmem, vmem),
        scratch_shapes=[
            *[pltpu.SMEM(value.shape, jnp.int32) for value in ints],
            *[pltpu.VMEM(value.shape, f32) for value in (pos, vel, mpos, mvel)],
            pltpu.VMEM((axes[0] * leaving, 8, slots), f32),
            pltpu.VMEM((leaving, 8, slots), f32),
            pltpu.VMEM((hx, sy, hz, slots, 48), bf16),
            pltpu.VMEM((hx, pairs, hz, slots, 96), bf16),
            pltpu.VMEM((sx, pairs, sz, 3, 48, wide), bf16),
            pltpu.VMEM((sx, pairs, sz, 3, 96, wide), bf16),
            pltpu.VMEM((hx, sy, hz, 16, wide), bf16),
            pltpu.VMEM((hx, pairs, hz, 32, wide), bf16),
            pltpu.SemaphoreType.DMA((27,)),
            pltpu.SemaphoreType.DMA((27,)),
            pltpu.SemaphoreType.DMA((2, axes[0])),
            pltpu.SemaphoreType.DMA((2, axes[0])),
            pltpu.SemaphoreType.DMA((8,)),
            pltpu.SemaphoreType.REGULAR((6,)),
            pltpu.VMEM((slots, wide), f32),
            pltpu.VMEM((2, 2 * slots, wide), bf16),
        ],
        compiler_params=pltpu.CompilerParams(
            collective_id=0,
            has_side_effects=True,
        ),
        name="pairs",
    )(*ints, pos, vel, mpos, mvel)


def kick(halo, speeds, sums):
    out = jax.ShapeDtypeStruct(speeds.shape, f32)
    vmem = pl.BlockSpec(memory_space=pltpu.VMEM)
    return pl.pallas_call(
        functools.partial(kick_kernel, speeds.shape[1:4]),
        out_shape=(out, out),
        in_specs=[vmem] * 3,
        out_specs=(vmem, vmem),
        compiler_params=pltpu.CompilerParams(vmem_limit_bytes=16 * 1024 * 1024),
        name="kick",
    )(halo, speeds, sums)


def per_device(
    positions, velocities, occupancy, mover_pos, mover_vel, mover_count, mover_owner, mover_cell
):
    slots, leaving = positions.shape[4], mover_pos.shape[1]
    halo, speeds, sums = pair_sums(
        occupancy,
        mover_count.reshape(leaving),
        mover_owner.reshape(leaving),
        mover_cell.reshape(leaving),
        positions,
        velocities,
        mover_pos.reshape(3, leaving, 1, slots),
        mover_vel.reshape(3, leaving, 1, slots),
    )
    return kick(halo, speeds, sums)


def solution(mesh):
    cells = P(None, "gx", "gy", "gz", None)
    labels = P("gx", "gy", "gz")
    return jax.shard_map(
        per_device,
        mesh=mesh,
        in_specs=(cells, cells, labels, cells, cells, labels, labels, labels),
        out_specs=(cells, cells),
        check_vma=False,
    )
```

```python
import functools

import jax
import jax.numpy as jnp
from jax import lax
from jax.experimental import pallas as pl
from jax.experimental.pallas import tpu as pltpu
from jax.sharding import PartitionSpec as P

eps_soft = 0.05
kick_step = 0.02
drift_step = 0.1
far_away = 1000.0

f32, bf16 = jnp.float32, jnp.bfloat16


def offsets(count):
    return sorted({0, 1 % count, count - 1})


def halo_steps():
    steps = [
        (dx, dy, dz)
        for dx in (-1, 0, 1)
        for dy in (-1, 0, 1)
        for dz in (-1, 0, 1)
        if (dx, dy, dz) != (0, 0, 0)
    ]
    return sorted(steps, key=lambda step: -sum(abs(d) for d in step))


def row_index(shape):
    return lax.broadcasted_iota(jnp.int32, shape, len(shape) - 2)


def split(value):
    high = value.astype(bf16).astype(f32)
    rest = value - high
    middle = rest.astype(bf16).astype(f32)
    return high, middle, rest - middle


def stack(high, middle, low):
    return jnp.concatenate([high, high, high, middle, middle, low], -2).astype(bf16)


def centre(dims, x, y):
    return x - 1 - 0.5 * dims[0], y - 1 - 0.5 * dims[1]


def pair_kernel(
    axes, dims, leaving, unroll, occ_h, count_h, owner_h, cell_h, pos_h, vel_h, mpos_h, mvel_h,
    halo_ref, velm_ref, total, occ_s, count_s, owner_s, cell_s, pos_ref, vel_ref, mpos_ref,
    mvel_ref, line, mov, left, left2, right, right2, src, src2, send, recv, msend, mrecv, fetch, known, ahead,
    behind
):
    nx, ny, nz = axes
    sx, sy, sz = dims
    hx, hy, hz = (size + 2 for size in dims)
    slots = pos_ref.shape[-1]
    fetches = [
        pltpu.make_async_copy(there, here, fetch.at[i])
        for i, (there, here) in enumerate([
            (mpos_h, mpos_ref), (mvel_h, mvel_ref), (count_h, count_s), (owner_h, owner_s),
            (cell_h, cell_s), (occ_h, occ_s), (pos_h, pos_ref), (vel_h, vel_ref),
        ])
    ]
    for copy in fetches:
        copy.start()
    me = [lax.axis_index(name) for name in ("gx", "gy", "gz")]

    def device(step):
        return tuple(lax.rem(m + s, n) for m, s, n in zip(me, step, axes))

    def along_line(body, start):
        if nx <= 4:
            for ox in range(start, nx):
                body(ox)
        else:
            lax.fori_loop(start, nx, lambda ox, carry: (body(ox), carry)[1], 0)

    def halo_copy(step):
        source, target = [], []
        for d, size in zip(step, dims):
            if d == 0:
                source.append(pl.ds(1, size))
                target.append(pl.ds(1, size))
            elif d == 1:
                source.append(pl.ds(size, 1))
                target.append(pl.ds(0, 1))
            else:
                source.append(pl.ds(1, 1))
                target.append(pl.ds(size + 1, 1))
        number = (step[0] + 1) * 9 + (step[1] + 1) * 3 + step[2] + 1
        return pltpu.make_async_remote_copy(
            src_ref=halo_ref.at[(*source, pl.ds(0, 3))],
            dst_ref=halo_ref.at[(*target, pl.ds(0, 3))],
            send_sem=send.at[number],
            recv_sem=recv.at[number],
            device_id=device([d % n for d, n in zip(step, axes)]),
            device_id_type=pl.DeviceIdType.MESH,
        )

    def mover_copy(ox, part):
        rows = pl.ds(4 * part, 4)
        return pltpu.make_async_remote_copy(
            src_ref=mov.at[:, rows],
            dst_ref=line.at[pl.ds(me[0] * leaving, leaving), rows],
            send_sem=msend.at[part, ox],
            recv_sem=mrecv.at[part, ox],
            device_id=device((ox, 0, 0)),
            device_id_type=pl.DeviceIdType.MESH,
        )

    tile = row_index((8, slots))

    def sources(x, y, z0, z1):
        ox, oy = centre(dims, x, y)
        shift = jnp.where(tile == 0, ox, jnp.where(tile == 1, oy, -0.5)).astype(f32)
        out = {}
        for z in range(z0, z1):
            extra = jnp.where(tile == 6, 1.0, jnp.where(tile == 7, float(z - 1 - sz // 2), 0.0))
            at = jnp.where(tile < 3, halo_ref[x, y, z] + shift, 0.0)
            high, middle, low = split(at + pltpu.roll(at * at, 3, 0) + extra.astype(f32))
            both = jnp.concatenate([high, middle], 0).astype(bf16)
            out[z] = stack(high, middle, low), jnp.concatenate([both, both], 1)
        return out

    def shared_columns(x, z0, z1):
        for y in range(1, sy + 1):
            for z, (keys, twice) in sources(x, y, z0, z1).items():
                left[x, y - 1, z] = keys.T
                src[x, y - 1, z] = twice

    def split_columns(x):
        for pair in range(sy // 2):
            low, up = sources(x, 2 * pair, 0, hz), sources(x, 2 * pair + 3, 0, hz)
            for z in range(hz):
                left2[x, pair, z] = jnp.concatenate([low[z][0], up[z][0]], 0).T
                src2[x, pair, z] = jnp.concatenate([low[z][1], up[z][1]], 0)

    def targets(x, pair, z):
        tiles = []
        for y in (2 * pair, 2 * pair + 1):
            ox, oy = centre(dims, x + 1, y + 1)
            shift = jnp.where(tile == 0, ox, jnp.where(tile == 1, oy, -0.5)).astype(f32)
            at = halo_ref[x + 1, y + 1, z + 1]
            tiles.append(jnp.where(at < 0.5 * far_away, at, 0.5) + shift)
        zero = jnp.zeros((48, slots), bf16)
        for e in (-1, 0, 1):
            keys = []
            for at in tiles:
                at = jnp.where(tile < 3, at - jnp.where(tile == 2, float(e), 0.0).astype(f32), 0.0)
                norm = jnp.sum(at * at, axis=0, keepdims=True) + eps_soft
                key = jnp.where(tile < 3, -2.0 * at, jnp.where(tile < 6, 1.0, norm))
                key = jnp.where(tile < 7, key, 0.0)
                high, middle, low = split(key)
                keys.append(
                    jnp.concatenate([high, middle, low, high, middle, high], 0).astype(bf16)
                )
            right[x, pair, z, e + 1] = jnp.concatenate(keys, 1)
            right2[x, pair, z, e + 1] = jnp.concatenate(
                [jnp.concatenate([keys[0], zero], 1), jnp.concatenate([zero, keys[1]], 1)], 0
            )

    def weights(t):
        y = lax.rsqrt(t)
        a = jnp.maximum((1.0 + eps_soft) - t, 0.0) * y
        w = a * a * y
        high = w.astype(bf16)
        return jnp.concatenate([high, (w - high.astype(f32)).astype(bf16)], 0)

    def accumulate(steps, sums):
        lag = 2

        def distances(n):
            return jnp.dot(steps[n][0][...], steps[n][1][...], preferred_element_type=f32)

        queue, ready = [distances(0)], []
        for n in range(len(steps) + lag):
            if n < len(steps):
                if n + 1 < len(steps):
                    queue.append(distances(n + 1))
                ready.append(weights(queue.pop(0)))
            if n >= lag:
                step = steps[n - lag]
                sums[step[3]] = sums[step[3]] + jnp.dot(
                    step[2][...], ready.pop(0), preferred_element_type=f32
                )
        return sums

    def steps_of(columns, shared, levels, x, pair, z, slot):
        steps = []
        for e in levels:
            for dx in columns:
                if shared:
                    for y in (2 * pair, 2 * pair + 1):
                        steps.append((
                            left.at[dx, y, z + e], right.at[x, pair, z, e], src.at[dx, y, z + e], slot
                        ))
                else:
                    steps.append((
                        left2.at[dx, pair, z + e], right2.at[x, pair, z, e],
                        src2.at[dx, pair, z + e], slot,
                    ))
        return steps

    def add(x, pair, z, value, shared, first=False):
        for half in range(2):
            rows = slice(0, 16) if shared else slice(16 * half, 16 * half + 16)
            part = value[rows, half * slots : (half + 1) * slots]
            if not first:
                part = part + total[x, pair, half, z]
            total[x, pair, half, z] = part

    def product(step):
        return jnp.dot(step[0][...], step[1][...], preferred_element_type=f32)

    def gather(step, weight):
        return jnp.dot(step[2][...], weight, preferred_element_type=f32)

    def phase(columns, shared, levels=(0, 1, 2), first=False, unroll=unroll):
        rounds, lag = sz // unroll, 2
        zero = jnp.zeros((16 if shared else 32, 2 * slots), f32)
        for x in range(sx):
            near_x = [dx for dx in columns if x <= dx <= x + 2]
            for pair in range(sy // 2):

                def group(i, x=x, pair=pair, near_x=near_x):
                    steps = []
                    for u in range(unroll):
                        steps += steps_of(near_x, shared, levels, x, pair, i * unroll + u, u)
                    return steps

                if rounds == 1:
                    sums = accumulate(group(0), [zero] * unroll)
                    for u in range(unroll):
                        add(x, pair, u, sums[u], shared, first)
                    continue

                ahead[...] = product(group(0)[0])
                for k in range(lag):
                    behind[k] = jnp.zeros(behind.shape[1:], bf16)

                def body(i, carry, x=x, pair=pair, group=group):
                    steps = group(i)
                    following = group(lax.rem(i + 1, rounds))[0]
                    before = group(lax.rem(i + rounds - 1, rounds))[-lag:]
                    sums, late = [zero] * unroll, zero
                    now, ready = ahead[...], []
                    for n in range(len(steps)):
                        then = product(steps[n + 1] if n + 1 < len(steps) else following)
                        ready.append(weights(now))
                        now = then
                        if n < lag:
                            late = late + gather(before[n], behind[n])
                        else:
                            step = steps[n - lag]
                            sums[step[3]] = sums[step[3]] + gather(step, ready.pop(0))
                    for k in range(lag):
                        behind[k] = ready[k]
                    ahead[...] = now
                    for u in range(unroll):
                        add(x, pair, i * unroll + u, sums[u], shared)
                    add(x, pair, lax.rem(i * unroll + sz - 1, sz), late, shared)
                    return carry

                lax.fori_loop(0, rounds, body, 0)
                late = zero
                for k, step in enumerate(group(rounds - 1)[-lag:]):
                    late = late + gather(step, behind[k])
                add(x, pair, sz - 1, late, shared)

    def arrive(which):
        for step in halo_steps():
            if which(*step):
                halo_copy(step).wait_recv()

    barrier = pltpu.get_barrier_semaphore()
    ys, zs = offsets(ny)[1:], offsets(nz)[1:]

    def greet(sem, step):
        pl.semaphore_signal(
            sem, inc=1, device_id=device(step), device_id_type=pl.DeviceIdType.MESH
        )

    for oz in zs:
        greet(barrier, (0, 0, oz))
    odd = me[1] % 2

    @pl.when(odd == 0)
    def _():
        for oy in ys:
            greet(barrier, (0, oy, 0))

    along_line(lambda ox: greet(barrier, (ox, 0, 0)), 1)

    for copy in fetches[:5]:
        copy.wait()
    lane = lax.broadcasted_iota(jnp.int32, (1, slots), 1)
    base = me[0] * (sx * sy * sz)
    for b in range(leaving):
        live = lane < count_s[b]
        rows = [jnp.where(live, mpos_ref[k, b], far_away) for k in range(3)]
        label = owner_s[b] * (sx * sy * sz) + cell_s[b]
        rows += [jnp.full((1, slots), label, jnp.int32).astype(f32)]
        rows += [mvel_ref[k, b] for k in range(3)]
        for k, row in enumerate(rows):
            mov[b, k : k + 1, :] = row
            line[me[0] * leaving + b, k : k + 1, :] = row

    pl.semaphore_wait(barrier, nx - 1 + len(zs) + odd * len(ys))
    along_line(lambda ox: mover_copy(ox, 0).start(), 1)

    @pl.when(odd == 1)
    def _():
        for i, oy in enumerate(ys):
            greet(known.at[i], (0, oy, 0))

    for i, oz in enumerate(zs):
        greet(known.at[2 + i], (0, 0, oz))

    for copy in fetches[5:]:
        copy.wait()
    sub = row_index((sz, slots))
    lanes = lax.broadcasted_iota(jnp.int32, (sz, slots), 1)
    planes, where = [], []
    for x in range(sx):
        for y in range(sy):
            counts = jnp.zeros((sz, slots), jnp.int32)
            for z in range(sz):
                counts = jnp.where(sub == z, occ_s[x, y, z], counts)
            live = lanes < counts
            planes.append(
                [jnp.where(live, pos_ref[k, x, y], far_away) for k in range(3)]
            )
            where.append((sub + (base + (x * sy + y) * sz)).astype(f32))
    along_line(lambda ox: mover_copy(ox, 0).wait_recv(), 1)

    def merge(first):
        def one(b, planes):
            label = line[b, pl.ds(3, 1), :]
            rows = [line[b, pl.ds(first + k, 1), :] for k in range(3)]
            return [
                [jnp.where(here == label, row, old) for row, old in zip(rows, plane)]
                for plane, here in zip(planes, where)
            ]

        return one

    def merged(first, planes):
        if nx <= 4:
            for b in range(nx * leaving):
                planes = merge(first)(b, planes)
            return planes
        return lax.fori_loop(0, nx * leaving, merge(first), planes)

    planes = merged(0, planes)

    flat = halo_ref.reshape((sx + 2) * (sy + 2) * (sz + 2) * 8, slots)
    for x in range(sx):
        for y in range(sy):
            first = (((x + 1) * (sy + 2) + y + 1) * (sz + 2) + 1) * 8
            for k in range(3):
                flat[pl.ds(first + k, sz, stride=8), :] = planes[x * sy + y][k]
    assert ny % 2 == 0

    def send_where(which):
        for step in halo_steps():
            if which(*step):
                halo_copy(step).start()

    send_where(lambda dx, dy, dz: abs(dx) + abs(dy) + abs(dz) == 1 and dy == 0)
    for i in range(len(zs)):
        pl.semaphore_wait(known.at[2 + i], 1)
    send_where(lambda dx, dy, dz: dx != 0 and dy == 0 and dz != 0)
    along_line(lambda ox: mover_copy(ox, 1).start(), 1)

    inner, outer = range(1, sx + 1), (0, sx + 1)
    for x in range(sx):
        for pair in range(sy // 2):
            for z in range(sz):
                targets(x, pair, z)
    for x in inner:
        shared_columns(x, 1, sz + 1)
    @pl.when(odd == 0)
    def _():
        for i, oy in enumerate(ys):
            pl.semaphore_wait(known.at[i], 1)
        for i, oy in enumerate(ys):
            greet(known.at[i], (0, oy, 0))

    @pl.when(odd == 1)
    def _():
        for i in range(len(ys)):
            pl.semaphore_wait(known.at[i], 1)

    for i, oz in enumerate(zs):
        greet(known.at[4 + i], (0, 0, oz))
    send_where(lambda dx, dy, dz: dx != 0 and dy != 0 and dz == 0)
    send_where(lambda dx, dy, dz: dx == 0 and dy != 0)
    phase(inner, True, (1,), True, sz)

    for i in range(len(zs)):
        pl.semaphore_wait(known.at[4 + i], 1)
    send_where(lambda dx, dy, dz: dx != 0 and dy != 0 and dz != 0)
    arrive(lambda dx, dy, dz: dx == 0 and dy == 0)
    for x in inner:
        shared_columns(x, 0, 1)
        shared_columns(x, sz + 1, sz + 2)
    phase(inner, True, (0, 2), False, sz)
    arrive(lambda dx, dy, dz: dx != 0 and dy == 0)
    for x in outer:
        shared_columns(x, 0, hz)
    phase(outer, True, (0, 1, 2), False, sz)
    along_line(lambda ox: mover_copy(ox, 1).wait(), 1)
    speeds = merged(4, [[vel_ref[k, x, y] for k in range(3)] for x in range(sx) for y in range(sy)])
    for x in range(sx):
        for y in range(sy):
            for k in range(3):
                velm_ref[k, x, y] = speeds[x * sy + y][k]
    arrive(lambda dx, dy, dz: dy != 0)
    for x in range(hx):
        split_columns(x)
    phase(range(hx), False, (0, 1, 2), False, sz)
    along_line(lambda ox: mover_copy(ox, 0).wait_send(), 1)
    for step in halo_steps():
        halo_copy(step).wait_send()


def kick_kernel(dims, halo_ref, vel_ref, total, npos_ref, nvel_ref):
    sx, sy, sz = dims
    hx, hy, hz = (size + 2 for size in dims)
    slots = halo_ref.shape[-1]
    flat = halo_ref.reshape(hx * hy * hz * 8, slots)
    for x in range(sx):
        for y in range(sy):
            sums = total.at[x, y // 2, y % 2].reshape(sz * 16, slots)

            def row(r, sums=sums):
                return sums[pl.ds(r, sz, stride=16), :]

            first = (((x + 1) * hy + y + 1) * hz + 1) * 8
            ox, oy = centre(dims, x + 1, y + 1)
            zat = (row_index((sz, slots)) - sz // 2).astype(f32)
            live = None
            for k, shift in enumerate((ox, oy, -0.5)):
                raw = flat[pl.ds(first + k, sz, stride=8), :]
                if k == 0:
                    live = raw < 0.5 * far_away
                high, middle, low = split(raw + shift)
                at, sum_s = high + middle, row(k) + row(8 + k)
                if k == 2:
                    at, sum_s = at + zat, sum_s + row(7)
                force = sum_s - at * row(6)
                vel = jnp.where(live, vel_ref[k, x, y] + kick_step * force, 0.0)
                nvel_ref[k, x, y] = vel
                npos_ref[k, x, y] = jnp.where(live, raw + drift_step * vel, 0.0)


def pair_sums(occupancy, count, owner, cell, pos, vel, mpos, mvel):
    axes = tuple(lax.axis_size(name) for name in ("gx", "gy", "gz"))
    sx, sy, sz = dims = pos.shape[1:4]
    leaving, slots = mpos.shape[1], mpos.shape[3]
    hx, hy, hz = padded = tuple(size + 2 for size in dims)
    pairs, wide = sy // 2, 2 * slots
    unroll = 4 if sz % 4 == 0 else 1
    vmem = pl.BlockSpec(memory_space=pltpu.VMEM)
    ints = (occupancy, count, owner, cell)
    return pl.pallas_call(
        functools.partial(pair_kernel, axes, dims, leaving, unroll),
        out_shape=(
            pltpu.VMEM((*padded, 8, slots), f32),
            pltpu.VMEM(vel.shape, f32),
            pltpu.VMEM((sx, pairs, 2, sz, 16, slots), f32),
        ),
        in_specs=[pl.BlockSpec(memory_space=pl.ANY)] * 8,
        out_specs=(vmem, vmem, vmem),
        scratch_shapes=[
            *[pltpu.SMEM(value.shape, jnp.int32) for value in ints],
            *[pltpu.VMEM(value.shape, f32) for value in (pos, vel, mpos, mvel)],
            pltpu.VMEM((axes[0] * leaving, 8, slots), f32),
            pltpu.VMEM((leaving, 8, slots), f32),
            pltpu.VMEM((hx, sy, hz, slots, 48), bf16),
            pltpu.VMEM((hx, pairs, hz, slots, 96), bf16),
            pltpu.VMEM((sx, pairs, sz, 3, 48, wide), bf16),
            pltpu.VMEM((sx, pairs, sz, 3, 96, wide), bf16),
            pltpu.VMEM((hx, sy, hz, 16, wide), bf16),
            pltpu.VMEM((hx, pairs, hz, 32, wide), bf16),
            pltpu.SemaphoreType.DMA((27,)),
            pltpu.SemaphoreType.DMA((27,)),
            pltpu.SemaphoreType.DMA((2, axes[0])),
            pltpu.SemaphoreType.DMA((2, axes[0])),
            pltpu.SemaphoreType.DMA((8,)),
            pltpu.SemaphoreType.REGULAR((6,)),
            pltpu.VMEM((slots, wide), f32),
            pltpu.VMEM((2, 2 * slots, wide), bf16),
        ],
        compiler_params=pltpu.CompilerParams(
            collective_id=0,
            has_side_effects=True,
        ),
        name="pairs",
    )(*ints, pos, vel, mpos, mvel)


def kick(halo, speeds, sums):
    out = jax.ShapeDtypeStruct(speeds.shape, f32)
    vmem = pl.BlockSpec(memory_space=pltpu.VMEM)
    return pl.pallas_call(
        functools.partial(kick_kernel, speeds.shape[1:4]),
        out_shape=(out, out),
        in_specs=[vmem] * 3,
        out_specs=(vmem, vmem),
        compiler_params=pltpu.CompilerParams(vmem_limit_bytes=16 * 1024 * 1024),
        name="kick",
    )(halo, speeds, sums)


def per_device(
    positions, velocities, occupancy, mover_pos, mover_vel, mover_count, mover_owner, mover_cell
):
    slots, leaving = positions.shape[4], mover_pos.shape[1]
    halo, speeds, sums = pair_sums(
        occupancy,
        mover_count.reshape(leaving),
        mover_owner.reshape(leaving),
        mover_cell.reshape(leaving),
        positions,
        velocities,
        mover_pos.reshape(3, leaving, 1, slots),
        mover_vel.reshape(3, leaving, 1, slots),
    )
    return kick(halo, speeds, sums)


def solution(mesh):
    cells = P(None, "gx", "gy", "gz", None)
    labels = P("gx", "gy", "gz")
    return jax.shard_map(
        per_device,
        mesh=mesh,
        in_specs=(cells, cells, labels, cells, cells, labels, labels, labels),
        out_specs=(cells, cells),
        check_vma=False,
    )
```
